8 devices in a mesh: col: 2 (over z, y), row: 4 (over x, core).
Axes of the slice: x: 2, y: 2, z: 1, core: 2. Of those that a mesh axis runs over, the one named last changes fastest.
Arguments:
- inter_mask: int32 [65536, 4096], P('row', 'col')
- emb_user: bfloat16 [65536, 256], P(('row', 'col'))
- emb_item: bfloat16 [4096, 256], P(('col', 'row'))
- triples: int32 [128, 3], replicated
Outputs:
- output 1: bfloat16 [65536, 256], P(('row', 'col'))
- output 2: bfloat16 [4096, 256], P(('col', 'row'))
- output 3: float32 [], replicated
All inputs are finite; a program needn't handle non-finite values.
Results may differ from the reference program's by a relative error of at most 0.00522126.
Values are sent between devices in bfloat16 or wider.
A program may use at most 1 GiB of HBM per device.

```python
import jax
import jax.numpy as jnp
from jax import lax

USERS = 65536
ITEMS = 4096
DIM = 256
LAYERS = 3
TRIPLES = 128
USER_DEGREE = 3


def draw_triples(trip_key):
    key_user, key_pos, key_neg = jax.random.split(trip_key, 3)
    row_pos = jnp.arange(TRIPLES)
    user_ids = jax.random.randint(key_user, (TRIPLES,), 0, USERS)
    pos_ids = jax.random.randint(key_pos, (TRIPLES,), 0, ITEMS)
    neg_ids = jax.random.randint(key_neg, (TRIPLES,), 0, ITEMS)
    user_ids = jnp.where(row_pos == 0, USERS - 1, jnp.where(row_pos == 1, 0, user_ids))
    pos_ids = jnp.where(row_pos == 0, ITEMS - 1, jnp.where(row_pos == 1, 0, pos_ids))
    neg_ids = jnp.where(row_pos == 0, 0, jnp.where(row_pos == 1, ITEMS - 1, neg_ids))
    return jnp.stack([user_ids, pos_ids, neg_ids], axis=1).astype(jnp.int32)


def setup_inputs(seed: int = 0) -> dict:
    base_key = jax.random.key(seed)
    key_mask, key_user, key_item, key_trip = jax.random.split(base_key, 4)
    raw_draw = jax.random.randint(key_mask, (USERS, ITEMS), 0, ITEMS)
    inter_mask = (raw_draw < USER_DEGREE).astype(jnp.int32)
    emb_user = jax.random.normal(key_user, (USERS, DIM), jnp.float32).astype(jnp.bfloat16)
    emb_item = jax.random.normal(key_item, (ITEMS, DIM), jnp.float32).astype(jnp.bfloat16)
    return {"inter_mask": inter_mask, "emb_user": emb_user, "emb_item": emb_item, "triples": draw_triples(key_trip)}


def reference(inter_mask, emb_user, emb_item, triples):
    deg_user = jnp.maximum(jnp.sum(inter_mask, axis=1), 1)
    deg_item = jnp.maximum(jnp.sum(inter_mask, axis=0), 1)
    scale_user = lax.rsqrt(deg_user.astype(jnp.float32))
    scale_item = lax.rsqrt(deg_item.astype(jnp.float32))
    norm_adj = (inter_mask.astype(jnp.float32) * scale_user[:, None] * scale_item[None, :]).astype(jnp.bfloat16)
    layer_user = emb_user
    layer_item = emb_item
    total_user = emb_user.astype(jnp.float32)
    total_item = emb_item.astype(jnp.float32)
    for layer_idx in range(LAYERS):
        next_user = jnp.dot(norm_adj, layer_item, preferred_element_type=jnp.float32).astype(jnp.bfloat16)
        next_item = lax.dot_general(norm_adj, layer_user, (((0,), (0,)), ((), ())), preferred_element_type=jnp.float32).astype(jnp.bfloat16)
        total_user = total_user + next_user.astype(jnp.float32)
        total_item = total_item + next_item.astype(jnp.float32)
        layer_user = next_user
        layer_item = next_item
    out_user = (total_user / (LAYERS + 1)).astype(jnp.bfloat16)
    out_item = (total_item / (LAYERS + 1)).astype(jnp.bfloat16)
    user_vec = jnp.take(out_user, triples[:, 0], axis=0).astype(jnp.float32)
    pos_vec = jnp.take(out_item, triples[:, 1], axis=0).astype(jnp.float32)
    neg_vec = jnp.take(out_item, triples[:, 2], axis=0).astype(jnp.float32)
    margin = jnp.sum(user_vec * pos_vec, axis=1) - jnp.sum(user_vec * neg_vec, axis=1)
    bpr_loss = jnp.mean(jax.nn.softplus(-margin))
    return out_user, out_item, bpr_loss
```

```python
import jax
import jax.numpy as jnp
from jax import lax
from jax.experimental import pallas as pl
from jax.experimental.pallas import tpu as pltpu
from jax.sharding import PartitionSpec as P


LAYERS = 3
LAST = LAYERS - 1
TAIL = (4, 3, 1)


ROW_BLOCK = 512
LANES = 128


def adj_kernel(base_ref, mask_ref, su_ref, sv_ref, table_ref, adj_ref, part_ref):
    def rows_of(r, carry):
        at = pl.multiple_of(r * LANES, LANES)
        row_scale = jnp.broadcast_to(su_ref[:, pl.ds(at, LANES)], (LANES, LANES)).T
        for j in range(0, mask_ref.shape[1], LANES):
            m = mask_ref[pl.ds(at, LANES), j:j + LANES].astype(jnp.float32)
            a = m * row_scale * sv_ref[:, j:j + LANES]
            adj_ref[pl.ds(at, LANES), j:j + LANES] = a.astype(jnp.bfloat16)
        return carry

    lax.fori_loop(0, ROW_BLOCK // LANES, rows_of, 0)
    part_ref[...] = jnp.dot(adj_ref[...], table_ref[...], preferred_element_type=jnp.float32)


def make_adj(mask, scale_user, scale_item, table, base, rows):
    items = mask.shape[1]
    dim = table.shape[1]
    return pl.pallas_call(
        adj_kernel,
        grid_spec=pltpu.PrefetchScalarGridSpec(
            num_scalar_prefetch=1,
            grid=(rows // ROW_BLOCK,),
            in_specs=[
                pl.BlockSpec((ROW_BLOCK, items), lambda i, b: (b[0] + i, 0)),
                pl.BlockSpec((1, ROW_BLOCK), lambda i, b: (0, b[0] + i)),
                pl.BlockSpec((1, items), lambda i, b: (0, 0)),
                pl.BlockSpec((items, dim), lambda i, b: (0, 0)),
            ],
            out_specs=[
                pl.BlockSpec((ROW_BLOCK, items), lambda i, b: (i, 0)),
                pl.BlockSpec((ROW_BLOCK, dim), lambda i, b: (i, 0)),
            ],
        ),
        out_shape=[
            jax.ShapeDtypeStruct((rows, items), jnp.bfloat16),
            jax.ShapeDtypeStruct((rows, dim), jnp.float32),
        ],
        cost_estimate=pl.CostEstimate(flops=2 * rows * items * dim, bytes_accessed=rows * items * 6, transcendentals=0),
    )((base // ROW_BLOCK).reshape(1), mask, scale_user.reshape(1, -1), scale_item.reshape(1, -1), table)


def users_kernel(adj_ref, table_ref, part_ref):
    part_ref[...] = jnp.dot(adj_ref[...], table_ref[...], preferred_element_type=jnp.float32)


def users_dot(adj, table):
    rows, items = adj.shape
    dim = table.shape[1]
    return pl.pallas_call(
        users_kernel,
        grid=(rows // ROW_BLOCK,),
        in_specs=[pl.BlockSpec((ROW_BLOCK, items), lambda i: (i, 0)), pl.BlockSpec((items, dim), lambda i: (0, 0))],
        out_specs=pl.BlockSpec((ROW_BLOCK, dim), lambda i: (i, 0)),
        out_shape=jax.ShapeDtypeStruct((rows, dim), jnp.float32),
        cost_estimate=pl.CostEstimate(flops=2 * rows * items * dim, bytes_accessed=rows * items * 2, transcendentals=0),
    )(adj, table)


def items_kernel(start_ref, adj_ref, user_ref, part_ref):
    @pl.when(pl.program_id(0) == 0)
    def _():
        part_ref[...] = start_ref[...]

    part_ref[...] += lax.dot_general(adj_ref[...], user_ref[...], (((0,), (0,)), ((), ())), preferred_element_type=jnp.float32)


def items_dot(adj, user, start):
    rows, items = adj.shape
    dim = user.shape[1]
    return pl.pallas_call(
        items_kernel,
        grid=(rows // ROW_BLOCK,),
        in_specs=[
            pl.BlockSpec((items, dim), lambda i: (0, 0)),
            pl.BlockSpec((ROW_BLOCK, items), lambda i: (i, 0)),
            pl.BlockSpec((ROW_BLOCK, dim), lambda i: (i, 0)),
        ],
        out_specs=pl.BlockSpec((items, dim), lambda i: (0, 0)),
        out_shape=jax.ShapeDtypeStruct((items, dim), jnp.float32),
        cost_estimate=pl.CostEstimate(flops=2 * rows * items * dim, bytes_accessed=rows * items * 2, transcendentals=0),
    )(start, adj, user)


def solution(mesh):
    row_count = mesh.shape["row"]
    col_count = mesh.shape["col"]
    f32 = jnp.float32
    bf16 = jnp.bfloat16

    def swap(value, axis, bit):
        pairs = [(i, i ^ bit) for i in range(mesh.shape[axis])]
        return lax.ppermute(value, axis, pairs)

    def cross(value):
        pairs = [(i, i ^ row_count ^ 2) for i in range(row_count * col_count)]
        value = lax.ppermute(value, ("col", "row"), pairs)
        return swap(value, "row", 2)

    def local_prog(mask_blk, user_shard, item_shard, triples):
        row_idx = lax.axis_index("row")
        col_idx = lax.axis_index("col")
        x_idx = row_idx >> 1
        core_idx = row_idx & 1
        rows = user_shard.shape[0]
        items = mask_blk.shape[1]
        dim = user_shard.shape[1]
        own_base = col_idx * rows
        oth_base = (1 - col_idx) * rows
        count = triples.shape[0]

        def gather_items(shard):
            other = swap(shard, "row", 2)
            first = x_idx == 0
            pair = jnp.stack([jnp.where(first, shard, other), jnp.where(first, other, shard)], axis=0)
            peer = swap(pair, "row", 1)
            first = core_idx == 0
            panel = jnp.stack([jnp.where(first, pair, peer), jnp.where(first, peer, pair)], axis=1)
            return panel.reshape(items, dim)

        def scatter_items(part):
            blocks = part.reshape(2, 2, items // 4, dim)
            keep = lax.dynamic_index_in_dim(blocks, core_idx, 1, keepdims=False)
            give = lax.dynamic_index_in_dim(blocks, 1 - core_idx, 1, keepdims=False)
            half = keep + swap(give, "row", 1)
            keep = lax.dynamic_index_in_dim(half, x_idx, 0, keepdims=False)
            give = lax.dynamic_index_in_dim(half, 1 - x_idx, 0, keepdims=False)
            return keep + swap(give, "row", 2)

        oth = swap(user_shard, "col", 1)
        panel = gather_items(item_shard)

        deg_user = jnp.sum(mask_blk, axis=1)
        deg_item = jnp.sum(mask_blk, axis=0)
        deg_user = jnp.maximum(deg_user + cross(deg_user), 1)
        deg_item = deg_item + swap(deg_item, "row", 1)
        deg_item = jnp.maximum(deg_item + swap(deg_item, "row", 2), 1)
        scale_user = lax.rsqrt(deg_user.astype(f32))
        scale_item = lax.rsqrt(deg_item.astype(f32))

        adj_oth, give0 = make_adj(mask_blk, scale_user, scale_item, panel, oth_base, rows)
        adj_own, mine0 = make_adj(mask_blk, scale_user, scale_item, panel, own_base, rows)

        own = user_shard
        item = item_shard
        own_list = [own]
        oth_list = [oth]
        item_list = [item]
        sizes = [rows * t // sum(TAIL) for t in TAIL]
        for k in range(LAYERS):
            give = give0 if k == 0 else users_dot(adj_oth, panel)
            if k == LAST:
                oth, _ = lax.optimization_barrier((oth, give))
            if k < LAST:
                got = [swap(give, "col", 1)]
            else:
                got, at = [], 0
                for n in sizes:
                    got.append(swap(give[at:at + n], "col", 1))
                    at += n
            mine = mine0 if k == 0 else users_dot(adj_own, panel)
            part = items_dot(adj_own, own, jnp.zeros((items, dim), f32))
            part = items_dot(adj_oth, oth, part)
            item = scatter_items(part).astype(bf16)
            item_list.append(item)
            if k < LAST:
                own = (mine + got[0]).astype(bf16)
                own_list.append(own)
                oth = swap(own, "col", 1)
                oth_list.append(oth)
                panel = gather_items(item)

        def mean(parts):
            total = parts[0].astype(f32)
            for p in parts[1:]:
                total = total + p.astype(f32)
            return (total / (LAYERS + 1)).astype(bf16)

        out_item = mean(item_list)

        def inside(ids, base, n):
            local = ids - base
            return (local >= 0) & (local < n), jnp.clip(local, 0, n - 1)

        user_ids = triples[:, 0]
        block = row_idx * col_count * rows
        own_in, own_at = inside(user_ids, block + own_base, rows)
        oth_in, oth_at = inside(user_ids, block + oth_base, rows)

        def pick(own_table, oth_table):
            a = jnp.take(own_table, own_at, axis=0)
            b = jnp.take(oth_table, oth_at, axis=0)
            return jnp.where(own_in[:, None], a, b)

        part_rows = pick(mine, give)
        last_rows = (part_rows + cross(part_rows)).astype(bf16)
        user_vec = mean([pick(a, b) for a, b in zip(own_list, oth_list)] + [last_rows]).astype(f32)
        table = gather_items(out_item)
        ids = jnp.concatenate([triples[:, 1], triples[:, 2]])
        item_in, item_at = inside(ids, col_idx * items, items)
        item_vec = jnp.take(table, item_at, axis=0).astype(f32).reshape(2, count, dim)
        dots = jnp.sum(user_vec[None] * item_vec, axis=2)
        dots = jnp.where((own_in | oth_in)[None] & item_in.reshape(2, count), dots, 0.0)
        dots = dots + swap(dots, "row", 1)
        dots = dots + swap(dots, "row", 2)
        dots = dots + cross(dots)
        bpr_loss = jnp.mean(jax.nn.softplus(dots[1] - dots[0]))

        at = 0
        out_user = None
        for i, n in enumerate(sizes):
            last = (mine[at:at + n] + got[i]).astype(bf16)
            piece = mean([t[at:at + n] for t in own_list] + [last])
            if out_user is None:
                out_user = jnp.pad(piece, ((0, rows - n), (0, 0)))
            else:
                out_user = lax.dynamic_update_slice(out_user, piece, (at, 0))
            at += n
        return out_user, out_item, bpr_loss

    return jax.shard_map(local_prog, mesh=mesh, in_specs=(P("row", "col"), P(("row", "col"), None), P(("col", "row"), None), P(None, None)), out_specs=(P(("row", "col"), None), P(("col", "row"), None), P()), check_vma=False)
```

```python
import jax
import jax.numpy as jnp
from jax import lax
from jax.experimental import pallas as pl
from jax.experimental.pallas import tpu as pltpu
from jax.sharding import PartitionSpec as P


LAYERS = 3
LAST = LAYERS - 1
TAIL = (8, 7, 1)
FIRST = 2


ROW_BLOCK = 512
LANES = 128


def adj_kernel(base_ref, mask_ref, su_ref, sv_ref, table_ref, *refs):
    adj_ref, part_ref = refs[-2:]

    def rows_of(r, carry):
        at = pl.multiple_of(r * LANES, LANES)
        row_scale = jnp.broadcast_to(su_ref[:, pl.ds(at, LANES)], (LANES, LANES)).T
        for j in range(0, mask_ref.shape[1], LANES):
            m = mask_ref[pl.ds(at, LANES), j:j + LANES].astype(jnp.float32)
            a = m * row_scale * sv_ref[:, j:j + LANES]
            adj_ref[pl.ds(at, LANES), j:j + LANES] = a.astype(jnp.bfloat16)
        return carry

    lax.fori_loop(0, ROW_BLOCK // LANES, rows_of, 0)
    part_ref[...] = jnp.dot(adj_ref[...], table_ref[...], preferred_element_type=jnp.float32)


def make_adj(mask, scale_user, scale_item, table, base, rows, piece, pieces, adj=None):
    items = mask.shape[1]
    dim = table.shape[1]
    blocks = rows // pieces // ROW_BLOCK
    first = piece * blocks
    extra = [] if adj is None else [adj]
    return pl.pallas_call(
        adj_kernel,
        grid_spec=pltpu.PrefetchScalarGridSpec(
            num_scalar_prefetch=1,
            grid=(blocks,),
            in_specs=[
                pl.BlockSpec((ROW_BLOCK, items), lambda i, b: (b[0] + i, 0)),
                pl.BlockSpec((1, ROW_BLOCK), lambda i, b: (0, b[0] + i)),
                pl.BlockSpec((1, items), lambda i, b: (0, 0)),
                pl.BlockSpec((items, dim), lambda i, b: (0, 0)),
            ] + [pl.BlockSpec(memory_space=pl.ANY) for _ in extra],
            out_specs=[
                pl.BlockSpec((ROW_BLOCK, items), lambda i, b: (first + i, 0)),
                pl.BlockSpec((ROW_BLOCK, dim), lambda i, b: (i, 0)),
            ],
        ),
        out_shape=[
            jax.ShapeDtypeStruct((rows, items), jnp.bfloat16),
            jax.ShapeDtypeStruct((rows // pieces, dim), jnp.float32),
        ],
        input_output_aliases={5: 0} if extra else {},
        cost_estimate=pl.CostEstimate(flops=2 * rows // pieces * items * dim, bytes_accessed=rows // pieces * items * 6, transcendentals=0),
    )((base // ROW_BLOCK + first).reshape(1), mask, scale_user.reshape(1, -1), scale_item.reshape(1, -1), table, *extra)


def users_kernel(adj_ref, table_ref, part_ref):
    part_ref[...] = jnp.dot(adj_ref[...], table_ref[...], preferred_element_type=jnp.float32)


def users_dot(adj, table):
    rows, items = adj.shape
    dim = table.shape[1]
    return pl.pallas_call(
        users_kernel,
        grid=(rows // ROW_BLOCK,),
        in_specs=[pl.BlockSpec((ROW_BLOCK, items), lambda i: (i, 0)), pl.BlockSpec((items, dim), lambda i: (0, 0))],
        out_specs=pl.BlockSpec((ROW_BLOCK, dim), lambda i: (i, 0)),
        out_shape=jax.ShapeDtypeStruct((rows, dim), jnp.float32),
        cost_estimate=pl.CostEstimate(flops=2 * rows * items * dim, bytes_accessed=rows * items * 2, transcendentals=0),
    )(adj, table)


def items_kernel(start_ref, adj_ref, user_ref, part_ref):
    @pl.when(pl.program_id(0) == 0)
    def _():
        part_ref[...] = start_ref[...]

    part_ref[...] += lax.dot_general(adj_ref[...], user_ref[...], (((0,), (0,)), ((), ())), preferred_element_type=jnp.float32)


def items_dot(adj, user, start):
    rows, items = adj.shape
    dim = user.shape[1]
    return pl.pallas_call(
        items_kernel,
        grid=(rows // ROW_BLOCK,),
        in_specs=[
            pl.BlockSpec((items, dim), lambda i: (0, 0)),
            pl.BlockSpec((ROW_BLOCK, items), lambda i: (i, 0)),
            pl.BlockSpec((ROW_BLOCK, dim), lambda i: (i, 0)),
        ],
        out_specs=pl.BlockSpec((items, dim), lambda i: (0, 0)),
        out_shape=jax.ShapeDtypeStruct((items, dim), jnp.float32),
        cost_estimate=pl.CostEstimate(flops=2 * rows * items * dim, bytes_accessed=rows * items * 2, transcendentals=0),
    )(start, adj, user)


def finish_kernel(done_ref, mine_ref, got_ref, *refs):
    tables, out_ref = refs[:-3], refs[-3]
    piece_ref, sem = refs[-2:]
    total = tables[0][...].astype(jnp.float32)
    for t in tables[1:]:
        total = total + t[...].astype(jnp.float32)
    total = total + (mine_ref[...] + got_ref[...]).astype(jnp.bfloat16).astype(jnp.float32)
    piece_ref[...] = (total / (LAYERS + 1)).astype(jnp.bfloat16)
    n = piece_ref.shape[0]
    copy = pltpu.make_async_copy(piece_ref, out_ref.at[pl.ds(out_ref.shape[0] - n, n)], sem)
    copy.start()
    copy.wait()


def finish(done, mine, got, tables, n):
    rows, dim = done.shape
    tail = pl.BlockSpec((n, dim), lambda i: (rows // n - 1, 0))
    return pl.pallas_call(
        finish_kernel,
        grid=(1,),
        in_specs=[pl.BlockSpec(memory_space=pltpu.HBM), tail, pl.BlockSpec((n, dim), lambda i: (0, 0))] + [tail for _ in tables],
        out_specs=pl.BlockSpec(memory_space=pltpu.HBM),
        out_shape=jax.ShapeDtypeStruct((rows, dim), jnp.bfloat16),
        input_output_aliases={0: 0},
        scratch_shapes=[pltpu.VMEM((n, dim), jnp.bfloat16), pltpu.SemaphoreType.DMA],
        cost_estimate=pl.CostEstimate(flops=8 * n * dim, bytes_accessed=16 * n * dim, transcendentals=0),
    )(done, mine, got, *tables)


def solution(mesh):
    row_count = mesh.shape["row"]
    col_count = mesh.shape["col"]
    f32 = jnp.float32
    bf16 = jnp.bfloat16

    def swap(value, axis, bit):
        pairs = [(i, i ^ bit) for i in range(mesh.shape[axis])]
        return lax.ppermute(value, axis, pairs)

    def cross(value):
        pairs = [(i, i ^ row_count ^ 2) for i in range(row_count * col_count)]
        value = lax.ppermute(value, ("col", "row"), pairs)
        return swap(value, "row", 2)

    def local_prog(mask_blk, user_shard, item_shard, triples):
        row_idx = lax.axis_index("row")
        col_idx = lax.axis_index("col")
        x_idx = row_idx >> 1
        core_idx = row_idx & 1
        rows = user_shard.shape[0]
        items = mask_blk.shape[1]
        dim = user_shard.shape[1]
        own_base = col_idx * rows
        oth_base = (1 - col_idx) * rows
        count = triples.shape[0]

        def gather_items(shard):
            other = swap(shard, "row", 2)
            first = x_idx == 0
            pair = jnp.stack([jnp.where(first, shard, other), jnp.where(first, other, shard)], axis=0)
            peer = swap(pair, "row", 1)
            first = core_idx == 0
            panel = jnp.stack([jnp.where(first, pair, peer), jnp.where(first, peer, pair)], axis=1)
            return panel.reshape(items, dim)

        def scatter_items(part):
            blocks = part.reshape(2, 2, items // 4, dim)
            keep = lax.dynamic_index_in_dim(blocks, core_idx, 1, keepdims=False)
            give = lax.dynamic_index_in_dim(blocks, 1 - core_idx, 1, keepdims=False)
            half = keep + swap(give, "row", 1)
            keep = lax.dynamic_index_in_dim(half, x_idx, 0, keepdims=False)
            give = lax.dynamic_index_in_dim(half, 1 - x_idx, 0, keepdims=False)
            return keep + swap(give, "row", 2)

        oth = swap(user_shard, "col", 1)
        panel = gather_items(item_shard)

        deg_user = jnp.sum(mask_blk, axis=1)
        deg_item = jnp.sum(mask_blk, axis=0)
        deg_user = jnp.maximum(deg_user + cross(deg_user), 1)
        deg_item = deg_item + swap(deg_item, "row", 1)
        deg_item = jnp.maximum(deg_item + swap(deg_item, "row", 2), 1)
        scale_user = lax.rsqrt(deg_user.astype(f32))
        scale_item = lax.rsqrt(deg_item.astype(f32))

        adj_oth = None
        give0 = []
        for i in range(FIRST):
            adj_oth, piece = make_adj(mask_blk, scale_user, scale_item, panel, oth_base, rows, i, FIRST, adj_oth)
            give0.append(piece)
        adj_own, mine0 = make_adj(mask_blk, scale_user, scale_item, panel, own_base, rows, 0, 1)

        own = user_shard
        item = item_shard
        own_list = [own]
        oth_list = [oth]
        item_list = [item]
        sizes = [rows * t // sum(TAIL) for t in TAIL]
        for k in range(LAYERS):
            give = give0 if k == 0 else users_dot(adj_oth, panel)
            if k == LAST:
                oth, _ = lax.optimization_barrier((oth, give))
            if k == 0:
                got = [jnp.concatenate([swap(g, "col", 1) for g in give], axis=0)]
            elif k < LAST:
                got = [swap(give, "col", 1)]
            else:
                got, at = [], 0
                for n in sizes:
                    got.append(swap(give[at:at + n], "col", 1))
                    at += n
            mine = mine0 if k == 0 else users_dot(adj_own, panel)
            part = items_dot(adj_own, own, jnp.zeros((items, dim), f32))
            part = items_dot(adj_oth, oth, part)
            item = scatter_items(part).astype(bf16)
            item_list.append(item)
            if k < LAST:
                own = (mine + got[0]).astype(bf16)
                own_list.append(own)
                oth = swap(own, "col", 1)
                oth_list.append(oth)
                panel = gather_items(item)

        def mean(parts):
            total = parts[0].astype(f32)
            for p in parts[1:]:
                total = total + p.astype(f32)
            return (total / (LAYERS + 1)).astype(bf16)

        out_item = mean(item_list)

        def inside(ids, base, n):
            local = ids - base
            return (local >= 0) & (local < n), jnp.clip(local, 0, n - 1)

        user_ids = triples[:, 0]
        block = row_idx * col_count * rows
        own_in, own_at = inside(user_ids, block + own_base, rows)
        oth_in, oth_at = inside(user_ids, block + oth_base, rows)

        def pick(own_table, oth_table):
            a = jnp.take(own_table, own_at, axis=0)
            b = jnp.take(oth_table, oth_at, axis=0)
            return jnp.where(own_in[:, None], a, b)

        part_rows = pick(mine, give)
        last_rows = (part_rows + cross(part_rows)).astype(bf16)
        user_vec = mean([pick(a, b) for a, b in zip(own_list, oth_list)] + [last_rows]).astype(f32)
        table = gather_items(out_item)
        ids = jnp.concatenate([triples[:, 1], triples[:, 2]])
        item_in, item_at = inside(ids, col_idx * items, items)
        item_vec = jnp.take(table, item_at, axis=0).astype(f32).reshape(2, count, dim)
        dots = jnp.sum(user_vec[None] * item_vec, axis=2)
        dots = jnp.where((own_in | oth_in)[None] & item_in.reshape(2, count), dots, 0.0)
        dots = dots + swap(dots, "row", 1)
        dots = dots + swap(dots, "row", 2)
        dots = dots + cross(dots)
        bpr_loss = jnp.mean(jax.nn.softplus(dots[1] - dots[0]))

        at = 0
        out_user = None
        for i, n in enumerate(sizes):
            if i == len(sizes) - 1:
                break
            last = (mine[at:at + n] + got[i]).astype(bf16)
            piece = mean([t[at:at + n] for t in own_list] + [last])
            if out_user is None:
                out_user = jnp.pad(piece, ((0, rows - n), (0, 0)))
            else:
                out_user = lax.dynamic_update_slice(out_user, piece, (at, 0))
            at += n
        out_user = finish(out_user, mine, got[-1], own_list, sizes[-1])
        return out_user, out_item, bpr_loss

    return jax.shard_map(local_prog, mesh=mesh, in_specs=(P("row", "col"), P(("row", "col"), None), P(("col", "row"), None), P(None, None)), out_specs=(P(("row", "col"), None), P(("col", "row"), None), P()), check_vma=False)
```

```python
import jax
import jax.numpy as jnp
from jax import lax
from jax.experimental import pallas as pl
from jax.experimental.pallas import tpu as pltpu
from jax.sharding import PartitionSpec as P


LAYERS = 3
LAST = LAYERS - 1
TAIL = (8, 7, 1)
FIRST = 2


ROW_BLOCK = 512
LANES = 128


def adj_kernel(base_ref, mask_ref, su_ref, sv_ref, table_ref, *refs):
    adj_ref, part_ref = refs[-2:]

    def rows_of(r, carry):
        at = pl.multiple_of(r * LANES, LANES)
        row_scale = jnp.broadcast_to(su_ref[:, pl.ds(at, LANES)], (LANES, LANES)).T
        for j in range(0, mask_ref.shape[1], LANES):
            m = mask_ref[pl.ds(at, LANES), j:j + LANES].astype(jnp.float32)
            a = m * row_scale * sv_ref[:, j:j + LANES]
            adj_ref[pl.ds(at, LANES), j:j + LANES] = a.astype(jnp.bfloat16)
        return carry

    lax.fori_loop(0, ROW_BLOCK // LANES, rows_of, 0)
    part_ref[...] = jnp.dot(adj_ref[...], table_ref[...], preferred_element_type=jnp.float32)


def make_adj(mask, scale_user, scale_item, table, base, rows, piece, pieces, adj=None):
    items = mask.shape[1]
    dim = table.shape[1]
    blocks = rows // pieces // ROW_BLOCK
    first = piece * blocks
    extra = [] if adj is None else [adj]
    return pl.pallas_call(
        adj_kernel,
        grid_spec=pltpu.PrefetchScalarGridSpec(
            num_scalar_prefetch=1,
            grid=(blocks,),
            in_specs=[
                pl.BlockSpec((ROW_BLOCK, items), lambda i, b: (b[0] + i, 0)),
                pl.BlockSpec((1, ROW_BLOCK), lambda i, b: (0, b[0] + i)),
                pl.BlockSpec((1, items), lambda i, b: (0, 0)),
                pl.BlockSpec((items, dim), lambda i, b: (0, 0)),
            ] + [pl.BlockSpec(memory_space=pl.ANY) for _ in extra],
            out_specs=[
                pl.BlockSpec((ROW_BLOCK, items), lambda i, b: (first + i, 0)),
                pl.BlockSpec((ROW_BLOCK, dim), lambda i, b: (i, 0)),
            ],
        ),
        out_shape=[
            jax.ShapeDtypeStruct((rows, items), jnp.bfloat16),
            jax.ShapeDtypeStruct((rows // pieces, dim), jnp.float32),
        ],
        input_output_aliases={5: 0} if extra else {},
        cost_estimate=pl.CostEstimate(flops=2 * rows // pieces * items * dim, bytes_accessed=rows // pieces * items * 6, transcendentals=0),
    )((base // ROW_BLOCK + first).reshape(1), mask, scale_user.reshape(1, -1), scale_item.reshape(1, -1), table, *extra)


def users_kernel(adj_ref, table_ref, part_ref):
    part_ref[...] = jnp.dot(adj_ref[...], table_ref[...], preferred_element_type=jnp.float32)


def users_dot(adj, table):
    rows, items = adj.shape
    dim = table.shape[1]
    return pl.pallas_call(
        users_kernel,
        grid=(rows // ROW_BLOCK,),
        in_specs=[pl.BlockSpec((ROW_BLOCK, items), lambda i: (i, 0)), pl.BlockSpec((items, dim), lambda i: (0, 0))],
        out_specs=pl.BlockSpec((ROW_BLOCK, dim), lambda i: (i, 0)),
        out_shape=jax.ShapeDtypeStruct((rows, dim), jnp.float32),
        cost_estimate=pl.CostEstimate(flops=2 * rows * items * dim, bytes_accessed=rows * items * 2, transcendentals=0),
    )(adj, table)


def items_kernel(start_ref, adj_ref, user_ref, part_ref):
    @pl.when(pl.program_id(0) == 0)
    def _():
        part_ref[...] = start_ref[...]

    part_ref[...] += lax.dot_general(adj_ref[...], user_ref[...], (((0,), (0,)), ((), ())), preferred_element_type=jnp.float32)


def items_dot(adj, user, start):
    rows, items = adj.shape
    dim = user.shape[1]
    return pl.pallas_call(
        items_kernel,
        grid=(rows // ROW_BLOCK,),
        in_specs=[
            pl.BlockSpec((items, dim), lambda i: (0, 0)),
            pl.BlockSpec((ROW_BLOCK, items), lambda i: (i, 0)),
            pl.BlockSpec((ROW_BLOCK, dim), lambda i: (i, 0)),
        ],
        out_specs=pl.BlockSpec((items, dim), lambda i: (0, 0)),
        out_shape=jax.ShapeDtypeStruct((items, dim), jnp.float32),
        cost_estimate=pl.CostEstimate(flops=2 * rows * items * dim, bytes_accessed=rows * items * 2, transcendentals=0),
    )(start, adj, user)


def finish_kernel(done_ref, mine_ref, got_ref, base_ref, out_ref, piece_ref, sem):
    last = (mine_ref[...] + got_ref[...]).astype(jnp.bfloat16).astype(jnp.float32)
    piece_ref[...] = ((base_ref[...] + last) / (LAYERS + 1)).astype(jnp.bfloat16)
    n = piece_ref.shape[0]
    copy = pltpu.make_async_copy(piece_ref, out_ref.at[pl.ds(out_ref.shape[0] - n, n)], sem)
    copy.start()
    copy.wait()


def finish(done, mine, got, base):
    rows, dim = done.shape
    n = got.shape[0]
    vmem = pl.BlockSpec(memory_space=pltpu.VMEM)
    return pl.pallas_call(
        finish_kernel,
        in_specs=[pl.BlockSpec(memory_space=pltpu.HBM), vmem, vmem, vmem],
        out_specs=pl.BlockSpec(memory_space=pltpu.HBM),
        out_shape=jax.ShapeDtypeStruct((rows, dim), jnp.bfloat16),
        input_output_aliases={0: 0},
        scratch_shapes=[pltpu.VMEM((n, dim), jnp.bfloat16), pltpu.SemaphoreType.DMA],
        cost_estimate=pl.CostEstimate(flops=8 * n * dim, bytes_accessed=16 * n * dim, transcendentals=0),
    )(done, mine, got, base)


def solution(mesh):
    row_count = mesh.shape["row"]
    col_count = mesh.shape["col"]
    f32 = jnp.float32
    bf16 = jnp.bfloat16

    def swap(value, axis, bit):
        pairs = [(i, i ^ bit) for i in range(mesh.shape[axis])]
        return lax.ppermute(value, axis, pairs)

    def cross(value):
        pairs = [(i, i ^ row_count ^ 2) for i in range(row_count * col_count)]
        value = lax.ppermute(value, ("col", "row"), pairs)
        return swap(value, "row", 2)

    def local_prog(mask_blk, user_shard, item_shard, triples):
        row_idx = lax.axis_index("row")
        col_idx = lax.axis_index("col")
        x_idx = row_idx >> 1
        core_idx = row_idx & 1
        rows = user_shard.shape[0]
        items = mask_blk.shape[1]
        dim = user_shard.shape[1]
        own_base = col_idx * rows
        oth_base = (1 - col_idx) * rows
        count = triples.shape[0]

        def gather_items(shard):
            other = swap(shard, "row", 2)
            first = x_idx == 0
            pair = jnp.stack([jnp.where(first, shard, other), jnp.where(first, other, shard)], axis=0)
            peer = swap(pair, "row", 1)
            first = core_idx == 0
            panel = jnp.stack([jnp.where(first, pair, peer), jnp.where(first, peer, pair)], axis=1)
            return panel.reshape(items, dim)

        def scatter_rows(part):
            blocks = part.reshape(2, 2, part.shape[0] // 4, part.shape[1])
            keep = lax.dynamic_index_in_dim(blocks, core_idx, 1, keepdims=False)
            give = lax.dynamic_index_in_dim(blocks, 1 - core_idx, 1, keepdims=False)
            half = keep + swap(give, "row", 1)
            keep = lax.dynamic_index_in_dim(half, x_idx, 0, keepdims=False)
            give = lax.dynamic_index_in_dim(half, 1 - x_idx, 0, keepdims=False)
            return keep + swap(give, "row", 2)

        oth = swap(user_shard, "col", 1)
        panel = gather_items(item_shard)

        deg_user = jnp.sum(mask_blk, axis=1)
        deg_item = jnp.sum(mask_blk, axis=0)
        deg_user = jnp.maximum(deg_user + cross(deg_user), 1)
        deg_item = deg_item + swap(deg_item, "row", 1)
        deg_item = jnp.maximum(deg_item + swap(deg_item, "row", 2), 1)
        scale_user = lax.rsqrt(deg_user.astype(f32))
        scale_item = lax.rsqrt(deg_item.astype(f32))

        adj_oth = None
        give0 = []
        for i in range(FIRST):
            adj_oth, piece = make_adj(mask_blk, scale_user, scale_item, panel, oth_base, rows, i, FIRST, adj_oth)
            give0.append(piece)
        adj_own, mine0 = make_adj(mask_blk, scale_user, scale_item, panel, own_base, rows, 0, 1)

        own = user_shard
        item = item_shard
        own_list = [own]
        oth_list = [oth]
        item_list = [item]
        sizes = [rows * t // sum(TAIL) for t in TAIL]
        for k in range(LAYERS):
            give = give0 if k == 0 else users_dot(adj_oth, panel)
            if k == LAST:
                oth, _ = lax.optimization_barrier((oth, give))
            if k == 0:
                got = [jnp.concatenate([swap(g, "col", 1) for g in give], axis=0)]
            elif k < LAST:
                got = [swap(give, "col", 1)]
            else:
                got, at = [], 0
                for n in sizes:
                    got.append(swap(give[at:at + n], "col", 1))
                    at += n
            mine = mine0 if k == 0 else users_dot(adj_own, panel)
            part = items_dot(adj_own, own, jnp.zeros((items, dim), f32))
            part = items_dot(adj_oth, oth, part)
            item = scatter_rows(part).astype(bf16)
            item_list.append(item)
            if k < LAST:
                own = (mine + got[0]).astype(bf16)
                own_list.append(own)
                oth = swap(own, "col", 1)
                oth_list.append(oth)
                panel = gather_items(item)

        def mean(parts):
            total = parts[0].astype(f32)
            for p in parts[1:]:
                total = total + p.astype(f32)
            return (total / (LAYERS + 1)).astype(bf16)

        out_item = mean(item_list)

        def inside(ids, base, n):
            local = ids - base
            return (local >= 0) & (local < n), jnp.clip(local, 0, n - 1)

        user_ids = triples[:, 0]
        block = row_idx * col_count * rows
        own_in, own_at = inside(user_ids, block + own_base, rows)
        oth_in, oth_at = inside(user_ids, block + oth_base, rows)

        def pick(own_table, oth_table):
            a = jnp.where(own_in[:, None], jnp.take(own_table, own_at, axis=0), 0)
            b = jnp.where(oth_in[:, None], jnp.take(oth_table, oth_at, axis=0), 0)
            return (a + b).astype(f32)

        def add_up(parts):
            total = parts[0].astype(f32)
            for p in parts[1:]:
                total = total + p.astype(f32)
            return total

        sums = add_up([pick(a, b) for a, b in zip(own_list, oth_list)])
        both = jnp.concatenate([pick(mine, give), sums], axis=1)
        picked = scatter_rows(both)
        part_rows = picked[:, :dim]
        last_rows = (part_rows + cross(part_rows)).astype(bf16)
        user_vec = mean([picked[:, dim:], last_rows]).astype(f32)
        table = gather_items(out_item)
        share = count // row_count
        mine_ids = lax.dynamic_slice(triples, (row_idx * share, 0), (share, 3))
        item_in, item_at = inside(mine_ids[:, 1:].T.reshape(-1), col_idx * items, items)
        item_vec = jnp.take(table, item_at, axis=0).astype(f32).reshape(2, share, dim)
        dots = jnp.sum(user_vec[None] * item_vec, axis=2)
        dots = jnp.where(item_in.reshape(2, share), dots, 0.0)
        dots = dots + cross(dots)
        loss_sum = jnp.sum(jax.nn.softplus(dots[1] - dots[0])).reshape(1)
        loss_sum = loss_sum + swap(loss_sum, "row", 1)
        other_sum = swap(loss_sum, "row", 2)
        bpr_loss = ((loss_sum + other_sum) / count).reshape(())

        at = 0
        out_user = None
        for i, n in enumerate(sizes):
            if i == len(sizes) - 1:
                break
            last = (mine[at:at + n] + got[i]).astype(bf16)
            piece = mean([t[at:at + n] for t in own_list] + [last])
            if out_user is None:
                out_user = jnp.pad(piece, ((0, rows - n), (0, 0)))
            else:
                out_user = lax.dynamic_update_slice(out_user, piece, (at, 0))
            at += n
        n = sizes[-1]
        out_user = finish(out_user, mine[rows - n:], got[-1], add_up([t[rows - n:] for t in own_list]))
        return out_user, out_item, bpr_loss

    return jax.shard_map(local_prog, mesh=mesh, in_specs=(P("row", "col"), P(("row", "col"), None), P(("col", "row"), None), P(None, None)), out_specs=(P(("row", "col"), None), P(("col", "row"), None), P()), check_vma=False)
```

```python
import jax
import jax.numpy as jnp
from jax import lax
from jax.experimental import pallas as pl
from jax.experimental.pallas import tpu as pltpu
from jax.sharding import PartitionSpec as P


LAYERS = 3
LAST = LAYERS - 1
TAIL = (8, 7, 1)
FIRST = 2


ROW_BLOCK = 512
LANES = 128


def adj_kernel(base_ref, mask_ref, su_ref, sv_ref, table_ref, *refs):
    adj_ref, part_ref = refs[-2:]

    def rows_of(r, carry):
        at = pl.multiple_of(r * LANES, LANES)
        row_scale = jnp.broadcast_to(su_ref[:, pl.ds(at, LANES)], (LANES, LANES)).T
        for j in range(0, mask_ref.shape[1], LANES):
            m = mask_ref[pl.ds(at, LANES), j:j + LANES].astype(jnp.float32)
            a = m * row_scale * sv_ref[:, j:j + LANES]
            adj_ref[pl.ds(at, LANES), j:j + LANES] = a.astype(jnp.bfloat16)
        return carry

    lax.fori_loop(0, ROW_BLOCK // LANES, rows_of, 0)
    part_ref[...] = jnp.dot(adj_ref[...], table_ref[...], preferred_element_type=jnp.float32)


def make_adj(mask, scale_user, scale_item, table, base, rows, piece, pieces, adj=None):
    items = mask.shape[1]
    dim = table.shape[1]
    blocks = rows // pieces // ROW_BLOCK
    first = piece * blocks
    extra = [] if adj is None else [adj]
    return pl.pallas_call(
        adj_kernel,
        grid_spec=pltpu.PrefetchScalarGridSpec(
            num_scalar_prefetch=1,
            grid=(blocks,),
            in_specs=[
                pl.BlockSpec((ROW_BLOCK, items), lambda i, b: (b[0] + i, 0)),
                pl.BlockSpec((1, ROW_BLOCK), lambda i, b: (0, b[0] + i)),
                pl.BlockSpec((1, items), lambda i, b: (0, 0)),
                pl.BlockSpec((items, dim), lambda i, b: (0, 0)),
            ] + [pl.BlockSpec(memory_space=pl.ANY) for _ in extra],
            out_specs=[
                pl.BlockSpec((ROW_BLOCK, items), lambda i, b: (first + i, 0)),
                pl.BlockSpec((ROW_BLOCK, dim), lambda i, b: (i, 0)),
            ],
        ),
        out_shape=[
            jax.ShapeDtypeStruct((rows, items), jnp.bfloat16),
            jax.ShapeDtypeStruct((rows // pieces, dim), jnp.float32),
        ],
        input_output_aliases={5: 0} if extra else {},
        cost_estimate=pl.CostEstimate(flops=2 * rows // pieces * items * dim, bytes_accessed=rows // pieces * items * 6, transcendentals=0),
    )((base // ROW_BLOCK + first).reshape(1), mask, scale_user.reshape(1, -1), scale_item.reshape(1, -1), table, *extra)


def users_kernel(adj_ref, table_ref, part_ref):
    part_ref[...] = jnp.dot(adj_ref[...], table_ref[...], preferred_element_type=jnp.float32)


def users_dot(adj, table):
    rows, items = adj.shape
    dim = table.shape[1]
    return pl.pallas_call(
        users_kernel,
        grid=(rows // ROW_BLOCK,),
        in_specs=[pl.BlockSpec((ROW_BLOCK, items), lambda i: (i, 0)), pl.BlockSpec((items, dim), lambda i: (0, 0))],
        out_specs=pl.BlockSpec((ROW_BLOCK, dim), lambda i: (i, 0)),
        out_shape=jax.ShapeDtypeStruct((rows, dim), jnp.float32),
        cost_estimate=pl.CostEstimate(flops=2 * rows * items * dim, bytes_accessed=rows * items * 2, transcendentals=0),
    )(adj, table)


def items_kernel(start_ref, adj_ref, user_ref, part_ref):
    @pl.when(pl.program_id(0) == 0)
    def _():
        part_ref[...] = start_ref[...]

    part_ref[...] += lax.dot_general(adj_ref[...], user_ref[...], (((0,), (0,)), ((), ())), preferred_element_type=jnp.float32)


def items_dot(adj, user, start):
    rows, items = adj.shape
    dim = user.shape[1]
    return pl.pallas_call(
        items_kernel,
        grid=(rows // ROW_BLOCK,),
        in_specs=[
            pl.BlockSpec((items, dim), lambda i: (0, 0)),
            pl.BlockSpec((ROW_BLOCK, items), lambda i: (i, 0)),
            pl.BlockSpec((ROW_BLOCK, dim), lambda i: (i, 0)),
        ],
        out_specs=pl.BlockSpec((items, dim), lambda i: (0, 0)),
        out_shape=jax.ShapeDtypeStruct((items, dim), jnp.float32),
        cost_estimate=pl.CostEstimate(flops=2 * rows * items * dim, bytes_accessed=rows * items * 2, transcendentals=0),
    )(start, adj, user)


PICK_BLOCK = 1024


def pick_kernel(own_id_ref, oth_id_ref, *refs):
    out_ref = refs[-1]
    sides = len(refs) // 2
    step = pl.program_id(0)

    @pl.when(step == 0)
    def _():
        out_ref[...] = jnp.zeros_like(out_ref)

    count = own_id_ref.shape[0]
    at = lax.broadcasted_iota(jnp.int32, (count, PICK_BLOCK), 1) + step * PICK_BLOCK
    dim = refs[0].shape[1]
    for id_ref, tables in ((own_id_ref, refs[:sides]), (oth_id_ref, refs[sides:-1])):
        chosen = jnp.where(id_ref[...] == at, 1.0, 0.0).astype(jnp.bfloat16)
        total = tables[1][...].astype(jnp.float32)
        for t in tables[2:]:
            total = total + t[...].astype(jnp.float32)
        for place, value in ((0, tables[0][...]), (dim, total)):
            for _ in range(3):
                part = value.astype(jnp.bfloat16)
                out_ref[:, place:place + dim] += jnp.dot(chosen, part, preferred_element_type=jnp.float32)
                value = value - part.astype(jnp.float32)


def pick_rows(own_id, oth_id, own_tables, oth_tables):
    rows, dim = own_tables[0].shape
    count = own_id.shape[0]
    ids = pl.BlockSpec((count, 1), lambda i: (0, 0))
    block = pl.BlockSpec((PICK_BLOCK, dim), lambda i: (i, 0))
    return pl.pallas_call(
        pick_kernel,
        grid=(rows // PICK_BLOCK,),
        in_specs=[ids, ids] + [block] * (len(own_tables) + len(oth_tables)),
        out_specs=pl.BlockSpec((count, 2 * dim), lambda i: (0, 0)),
        out_shape=jax.ShapeDtypeStruct((count, 2 * dim), jnp.float32),
        cost_estimate=pl.CostEstimate(flops=24 * count * rows * dim, bytes_accessed=20 * rows * dim, transcendentals=0),
    )(own_id.reshape(count, 1), oth_id.reshape(count, 1), *own_tables, *oth_tables)


def finish_kernel(done_ref, mine_ref, got_ref, base_ref, out_ref, piece_ref, sem):
    last = (mine_ref[...] + got_ref[...]).astype(jnp.bfloat16).astype(jnp.float32)
    piece_ref[...] = ((base_ref[...] + last) / (LAYERS + 1)).astype(jnp.bfloat16)
    n = piece_ref.shape[0]
    copy = pltpu.make_async_copy(piece_ref, out_ref.at[pl.ds(out_ref.shape[0] - n, n)], sem)
    copy.start()
    copy.wait()


def finish(done, mine, got, base):
    rows, dim = done.shape
    n = got.shape[0]
    vmem = pl.BlockSpec(memory_space=pltpu.VMEM)
    return pl.pallas_call(
        finish_kernel,
        in_specs=[pl.BlockSpec(memory_space=pltpu.HBM), vmem, vmem, vmem],
        out_specs=pl.BlockSpec(memory_space=pltpu.HBM),
        out_shape=jax.ShapeDtypeStruct((rows, dim), jnp.bfloat16),
        input_output_aliases={0: 0},
        scratch_shapes=[pltpu.VMEM((n, dim), jnp.bfloat16), pltpu.SemaphoreType.DMA],
        cost_estimate=pl.CostEstimate(flops=8 * n * dim, bytes_accessed=16 * n * dim, transcendentals=0),
    )(done, mine, got, base)


def solution(mesh):
    row_count = mesh.shape["row"]
    col_count = mesh.shape["col"]
    f32 = jnp.float32
    bf16 = jnp.bfloat16

    def swap(value, axis, bit):
        pairs = [(i, i ^ bit) for i in range(mesh.shape[axis])]
        return lax.ppermute(value, axis, pairs)

    def cross(value):
        pairs = [(i, i ^ row_count ^ 2) for i in range(row_count * col_count)]
        value = lax.ppermute(value, ("col", "row"), pairs)
        return swap(value, "row", 2)

    def local_prog(mask_blk, user_shard, item_shard, triples):
        row_idx = lax.axis_index("row")
        col_idx = lax.axis_index("col")
        x_idx = row_idx >> 1
        core_idx = row_idx & 1
        rows = user_shard.shape[0]
        items = mask_blk.shape[1]
        dim = user_shard.shape[1]
        own_base = col_idx * rows
        oth_base = (1 - col_idx) * rows
        count = triples.shape[0]

        def gather_items(shard):
            other = swap(shard, "row", 2)
            first = x_idx == 0
            pair = jnp.stack([jnp.where(first, shard, other), jnp.where(first, other, shard)], axis=0)
            peer = swap(pair, "row", 1)
            first = core_idx == 0
            panel = jnp.stack([jnp.where(first, pair, peer), jnp.where(first, peer, pair)], axis=1)
            return panel.reshape(items, dim)

        def scatter_rows(part):
            blocks = part.reshape(2, 2, part.shape[0] // 4, part.shape[1])
            keep = lax.dynamic_index_in_dim(blocks, core_idx, 1, keepdims=False)
            give = lax.dynamic_index_in_dim(blocks, 1 - core_idx, 1, keepdims=False)
            half = keep + swap(give, "row", 1)
            keep = lax.dynamic_index_in_dim(half, x_idx, 0, keepdims=False)
            give = lax.dynamic_index_in_dim(half, 1 - x_idx, 0, keepdims=False)
            return keep + swap(give, "row", 2)

        oth = swap(user_shard, "col", 1)
        panel = gather_items(item_shard)

        deg_user = jnp.sum(mask_blk, axis=1)
        deg_item = jnp.sum(mask_blk, axis=0)
        deg_user = jnp.maximum(deg_user + cross(deg_user), 1)
        deg_item = deg_item + swap(deg_item, "row", 1)
        deg_item = jnp.maximum(deg_item + swap(deg_item, "row", 2), 1)
        scale_user = lax.rsqrt(deg_user.astype(f32))
        scale_item = lax.rsqrt(deg_item.astype(f32))

        adj_oth = None
        give0 = []
        for i in range(FIRST):
            adj_oth, piece = make_adj(mask_blk, scale_user, scale_item, panel, oth_base, rows, i, FIRST, adj_oth)
            give0.append(piece)
        adj_own, mine0 = make_adj(mask_blk, scale_user, scale_item, panel, own_base, rows, 0, 1)

        own = user_shard
        item = item_shard
        own_list = [own]
        oth_list = [oth]
        item_list = [item]
        sizes = [rows * t // sum(TAIL) for t in TAIL]
        for k in range(LAYERS):
            give = give0 if k == 0 else users_dot(adj_oth, panel)
            if k == LAST:
                oth, _ = lax.optimization_barrier((oth, give))
            if k == 0:
                got = [jnp.concatenate([swap(g, "col", 1) for g in give], axis=0)]
            elif k < LAST:
                got = [swap(give, "col", 1)]
            else:
                got, at = [], 0
                for n in sizes:
                    got.append(swap(give[at:at + n], "col", 1))
                    at += n
            mine = mine0 if k == 0 else users_dot(adj_own, panel)
            part = items_dot(adj_own, own, jnp.zeros((items, dim), f32))
            part = items_dot(adj_oth, oth, part)
            item = scatter_rows(part).astype(bf16)
            item_list.append(item)
            if k < LAST:
                own = (mine + got[0]).astype(bf16)
                own_list.append(own)
                oth = swap(own, "col", 1)
                oth_list.append(oth)
                panel = gather_items(item)

        def mean(parts):
            total = parts[0].astype(f32)
            for p in parts[1:]:
                total = total + p.astype(f32)
            return (total / (LAYERS + 1)).astype(bf16)

        out_item = mean(item_list)

        def inside(ids, base, n):
            local = ids - base
            return (local >= 0) & (local < n), jnp.clip(local, 0, n - 1)

        user_ids = triples[:, 0]
        block = row_idx * col_count * rows
        own_in, own_at = inside(user_ids, block + own_base, rows)
        oth_in, oth_at = inside(user_ids, block + oth_base, rows)

        def add_up(parts):
            total = parts[0].astype(f32)
            for p in parts[1:]:
                total = total + p.astype(f32)
            return total

        own_id = jnp.where(own_in, own_at, -1)
        oth_id = jnp.where(oth_in, oth_at, -1)
        both = pick_rows(own_id, oth_id, [mine] + own_list, [give] + oth_list)
        picked = scatter_rows(both)
        part_rows = picked[:, :dim]
        last_rows = (part_rows + cross(part_rows)).astype(bf16)
        user_vec = mean([picked[:, dim:], last_rows]).astype(f32)
        table = gather_items(out_item)
        share = count // row_count
        mine_ids = lax.dynamic_slice(triples, (row_idx * share, 0), (share, 3))
        item_in, item_at = inside(mine_ids[:, 1:].T.reshape(-1), col_idx * items, items)
        item_vec = jnp.take(table, item_at, axis=0).astype(f32).reshape(2, share, dim)
        dots = jnp.sum(user_vec[None] * item_vec, axis=2)
        dots = jnp.where(item_in.reshape(2, share), dots, 0.0)
        dots = dots + cross(dots)
        loss_sum = jnp.sum(jax.nn.softplus(dots[1] - dots[0])).reshape(1)
        loss_sum = loss_sum + swap(loss_sum, "row", 1)
        other_sum = swap(loss_sum, "row", 2)
        bpr_loss = ((loss_sum + other_sum) / count).reshape(())

        at = 0
        out_user = None
        for i, n in enumerate(sizes):
            if i == len(sizes) - 1:
                break
            last = (mine[at:at + n] + got[i]).astype(bf16)
            piece = mean([t[at:at + n] for t in own_list] + [last])
            if out_user is None:
                out_user = jnp.pad(piece, ((0, rows - n), (0, 0)))
            else:
                out_user = lax.dynamic_update_slice(out_user, piece, (at, 0))
            at += n
        n = sizes[-1]
        out_user = finish(out_user, mine[rows - n:], got[-1], add_up([t[rows - n:] for t in own_list]))
        return out_user, out_item, bpr_loss

    return jax.shard_map(local_prog, mesh=mesh, in_specs=(P("row", "col"), P(("row", "col"), None), P(("col", "row"), None), P(None, None)), out_specs=(P(("row", "col"), None), P(("col", "row"), None), P()), check_vma=False)
```

```python
import jax
import jax.numpy as jnp
from jax import lax
from jax.experimental import pallas as pl
from jax.experimental.pallas import tpu as pltpu
from jax.sharding import PartitionSpec as P


LAYERS = 3
LAST = LAYERS - 1
TAIL = (8, 7, 1)
FIRST = 2


ROW_BLOCK = 512
LANES = 128


def adj_kernel(base_ref, mask_ref, su_ref, sv_ref, table_ref, *refs):
    adj_ref, part_ref = refs[-2:]

    def rows_of(r, carry):
        at = pl.multiple_of(r * LANES, LANES)
        row_scale = jnp.broadcast_to(su_ref[:, pl.ds(at, LANES)], (LANES, LANES)).T
        for j in range(0, mask_ref.shape[1], LANES):
            m = mask_ref[pl.ds(at, LANES), j:j + LANES].astype(jnp.float32)
            a = m * row_scale * sv_ref[:, j:j + LANES]
            adj_ref[pl.ds(at, LANES), j:j + LANES] = a.astype(jnp.bfloat16)
        return carry

    lax.fori_loop(0, ROW_BLOCK // LANES, rows_of, 0)
    part_ref[...] = jnp.dot(adj_ref[...], table_ref[...], preferred_element_type=jnp.float32)


def make_adj(mask, scale_user, scale_item, table, base, rows, piece, pieces, adj=None):
    items = mask.shape[1]
    dim = table.shape[1]
    blocks = rows // pieces // ROW_BLOCK
    first = piece * blocks
    extra = [] if adj is None else [adj]
    return pl.pallas_call(
        adj_kernel,
        grid_spec=pltpu.PrefetchScalarGridSpec(
            num_scalar_prefetch=1,
            grid=(blocks,),
            in_specs=[
                pl.BlockSpec((ROW_BLOCK, items), lambda i, b: (b[0] + i, 0)),
                pl.BlockSpec((1, ROW_BLOCK), lambda i, b: (0, b[0] + i)),
                pl.BlockSpec((1, items), lambda i, b: (0, 0)),
                pl.BlockSpec((items, dim), lambda i, b: (0, 0)),
            ] + [pl.BlockSpec(memory_space=pl.ANY) for _ in extra],
            out_specs=[
                pl.BlockSpec((ROW_BLOCK, items), lambda i, b: (first + i, 0)),
                pl.BlockSpec((ROW_BLOCK, dim), lambda i, b: (i, 0)),
            ],
        ),
        out_shape=[
            jax.ShapeDtypeStruct((rows, items), jnp.bfloat16),
            jax.ShapeDtypeStruct((rows // pieces, dim), jnp.float32),
        ],
        input_output_aliases={5: 0} if extra else {},
        cost_estimate=pl.CostEstimate(flops=2 * rows // pieces * items * dim, bytes_accessed=rows // pieces * items * 6, transcendentals=0),
    )((base // ROW_BLOCK + first).reshape(1), mask, scale_user.reshape(1, -1), scale_item.reshape(1, -1), table, *extra)


def users_kernel(adj_ref, table_ref, part_ref):
    part_ref[...] = jnp.dot(adj_ref[...], table_ref[...], preferred_element_type=jnp.float32)


def users_dot(adj, table, first=0, rows=None):
    items = adj.shape[1]
    rows = adj.shape[0] if rows is None else rows
    dim = table.shape[1]
    at = first // ROW_BLOCK
    return pl.pallas_call(
        users_kernel,
        grid=(rows // ROW_BLOCK,),
        in_specs=[pl.BlockSpec((ROW_BLOCK, items), lambda i: (at + i, 0)), pl.BlockSpec((items, dim), lambda i: (0, 0))],
        out_specs=pl.BlockSpec((ROW_BLOCK, dim), lambda i: (i, 0)),
        out_shape=jax.ShapeDtypeStruct((rows, dim), jnp.float32),
        cost_estimate=pl.CostEstimate(flops=2 * rows * items * dim, bytes_accessed=rows * items * 2, transcendentals=0),
    )(adj, table)


def items_kernel(start_ref, adj_ref, user_ref, part_ref):
    @pl.when(pl.program_id(0) == 0)
    def _():
        part_ref[...] = start_ref[...]

    part_ref[...] += lax.dot_general(adj_ref[...], user_ref[...], (((0,), (0,)), ((), ())), preferred_element_type=jnp.float32)


def items_dot(adj, user, start):
    rows, items = adj.shape
    dim = user.shape[1]
    return pl.pallas_call(
        items_kernel,
        grid=(rows // ROW_BLOCK,),
        in_specs=[
            pl.BlockSpec((items, dim), lambda i: (0, 0)),
            pl.BlockSpec((ROW_BLOCK, items), lambda i: (i, 0)),
            pl.BlockSpec((ROW_BLOCK, dim), lambda i: (i, 0)),
        ],
        out_specs=pl.BlockSpec((items, dim), lambda i: (0, 0)),
        out_shape=jax.ShapeDtypeStruct((items, dim), jnp.float32),
        cost_estimate=pl.CostEstimate(flops=2 * rows * items * dim, bytes_accessed=rows * items * 2, transcendentals=0),
    )(start, adj, user)


PICK_BLOCK = 1024


def pick_kernel(own_id_ref, oth_id_ref, *refs):
    out_ref = refs[-1]
    sides = len(refs) // 2
    step = pl.program_id(0)

    @pl.when(step == 0)
    def _():
        out_ref[...] = jnp.zeros_like(out_ref)

    count = own_id_ref.shape[0]
    at = lax.broadcasted_iota(jnp.int32, (count, PICK_BLOCK), 1) + step * PICK_BLOCK
    dim = refs[0].shape[1]
    for id_ref, tables in ((own_id_ref, refs[:sides]), (oth_id_ref, refs[sides:-1])):
        chosen = jnp.where(id_ref[...] == at, 1.0, 0.0).astype(jnp.bfloat16)
        total = tables[1][...].astype(jnp.float32)
        for t in tables[2:]:
            total = total + t[...].astype(jnp.float32)
        for place, value in ((0, tables[0][...]), (dim, total)):
            for _ in range(3):
                part = value.astype(jnp.bfloat16)
                out_ref[:, place:place + dim] += jnp.dot(chosen, part, preferred_element_type=jnp.float32)
                value = value - part.astype(jnp.float32)


def pick_rows(own_id, oth_id, own_tables, oth_tables):
    rows, dim = own_tables[0].shape
    count = own_id.shape[0]
    ids = pl.BlockSpec((count, 1), lambda i: (0, 0))
    block = pl.BlockSpec((PICK_BLOCK, dim), lambda i: (i, 0))
    return pl.pallas_call(
        pick_kernel,
        grid=(rows // PICK_BLOCK,),
        in_specs=[ids, ids] + [block] * (len(own_tables) + len(oth_tables)),
        out_specs=pl.BlockSpec((count, 2 * dim), lambda i: (0, 0)),
        out_shape=jax.ShapeDtypeStruct((count, 2 * dim), jnp.float32),
        cost_estimate=pl.CostEstimate(flops=24 * count * rows * dim, bytes_accessed=20 * rows * dim, transcendentals=0),
    )(own_id.reshape(count, 1), oth_id.reshape(count, 1), *own_tables, *oth_tables)


def finish_kernel(done_ref, mine_ref, got_ref, base_ref, out_ref, piece_ref, sem):
    last = (mine_ref[...] + got_ref[...]).astype(jnp.bfloat16).astype(jnp.float32)
    piece_ref[...] = ((base_ref[...] + last) / (LAYERS + 1)).astype(jnp.bfloat16)
    n = piece_ref.shape[0]
    copy = pltpu.make_async_copy(piece_ref, out_ref.at[pl.ds(out_ref.shape[0] - n, n)], sem)
    copy.start()
    copy.wait()


def finish(done, mine, got, base):
    rows, dim = done.shape
    n = got.shape[0]
    vmem = pl.BlockSpec(memory_space=pltpu.VMEM)
    return pl.pallas_call(
        finish_kernel,
        in_specs=[pl.BlockSpec(memory_space=pltpu.HBM), vmem, vmem, vmem],
        out_specs=pl.BlockSpec(memory_space=pltpu.HBM),
        out_shape=jax.ShapeDtypeStruct((rows, dim), jnp.bfloat16),
        input_output_aliases={0: 0},
        scratch_shapes=[pltpu.VMEM((n, dim), jnp.bfloat16), pltpu.SemaphoreType.DMA],
        cost_estimate=pl.CostEstimate(flops=8 * n * dim, bytes_accessed=16 * n * dim, transcendentals=0),
    )(done, mine, got, base)


def solution(mesh):
    row_count = mesh.shape["row"]
    col_count = mesh.shape["col"]
    f32 = jnp.float32
    bf16 = jnp.bfloat16

    def swap(value, axis, bit):
        pairs = [(i, i ^ bit) for i in range(mesh.shape[axis])]
        return lax.ppermute(value, axis, pairs)

    def cross(value):
        pairs = [(i, i ^ row_count ^ 2) for i in range(row_count * col_count)]
        value = lax.ppermute(value, ("col", "row"), pairs)
        return swap(value, "row", 2)

    def local_prog(mask_blk, user_shard, item_shard, triples):
        row_idx = lax.axis_index("row")
        col_idx = lax.axis_index("col")
        x_idx = row_idx >> 1
        core_idx = row_idx & 1
        rows = user_shard.shape[0]
        items = mask_blk.shape[1]
        dim = user_shard.shape[1]
        own_base = col_idx * rows
        oth_base = (1 - col_idx) * rows
        count = triples.shape[0]

        def gather_items(shard):
            other = swap(shard, "row", 2)
            first = x_idx == 0
            pair = jnp.stack([jnp.where(first, shard, other), jnp.where(first, other, shard)], axis=0)
            peer = swap(pair, "row", 1)
            first = core_idx == 0
            panel = jnp.stack([jnp.where(first, pair, peer), jnp.where(first, peer, pair)], axis=1)
            return panel.reshape(items, dim)

        def scatter_rows(part):
            blocks = part.reshape(2, 2, part.shape[0] // 4, part.shape[1])
            keep = lax.dynamic_index_in_dim(blocks, core_idx, 1, keepdims=False)
            give = lax.dynamic_index_in_dim(blocks, 1 - core_idx, 1, keepdims=False)
            half = keep + swap(give, "row", 1)
            keep = lax.dynamic_index_in_dim(half, x_idx, 0, keepdims=False)
            give = lax.dynamic_index_in_dim(half, 1 - x_idx, 0, keepdims=False)
            return keep + swap(give, "row", 2)

        oth = swap(user_shard, "col", 1)
        panel = gather_items(item_shard)

        deg_user = jnp.sum(mask_blk, axis=1)
        deg_item = jnp.sum(mask_blk, axis=0)
        deg_user = jnp.maximum(deg_user + cross(deg_user), 1)
        deg_item = deg_item + swap(deg_item, "row", 1)
        deg_item = jnp.maximum(deg_item + swap(deg_item, "row", 2), 1)
        scale_user = lax.rsqrt(deg_user.astype(f32))
        scale_item = lax.rsqrt(deg_item.astype(f32))

        adj_oth = None
        give0 = []
        for i in range(FIRST):
            adj_oth, piece = make_adj(mask_blk, scale_user, scale_item, panel, oth_base, rows, i, FIRST, adj_oth)
            give0.append(piece)
        adj_own, mine0 = make_adj(mask_blk, scale_user, scale_item, panel, own_base, rows, 0, 1)

        own = user_shard
        item = item_shard
        own_list = [own]
        oth_list = [oth]
        item_list = [item]
        sizes = [rows * t // sum(TAIL) for t in TAIL]
        for k in range(LAYERS):
            if k == 0:
                got = [jnp.concatenate([swap(g, "col", 1) for g in give0], axis=0)]
            elif k < LAST:
                give = users_dot(adj_oth, panel)
                got = [swap(give, "col", 1)]
            else:
                got, give, at = [], [], 0
                for n in sizes:
                    give.append(users_dot(adj_oth, panel, at, n))
                    got.append(swap(give[-1], "col", 1))
                    at += n
                oth, _ = lax.optimization_barrier((oth, give[-1]))
                give = jnp.concatenate(give, axis=0)
            mine = mine0 if k == 0 else users_dot(adj_own, panel)
            part = items_dot(adj_own, own, jnp.zeros((items, dim), f32))
            part = items_dot(adj_oth, oth, part)
            item = scatter_rows(part).astype(bf16)
            item_list.append(item)
            if k < LAST:
                own = (mine + got[0]).astype(bf16)
                own_list.append(own)
                oth = swap(own, "col", 1)
                oth_list.append(oth)
                panel = gather_items(item)

        def mean(parts):
            total = parts[0].astype(f32)
            for p in parts[1:]:
                total = total + p.astype(f32)
            return (total / (LAYERS + 1)).astype(bf16)

        out_item = mean(item_list)

        def inside(ids, base, n):
            local = ids - base
            return (local >= 0) & (local < n), jnp.clip(local, 0, n - 1)

        user_ids = triples[:, 0]
        block = row_idx * col_count * rows
        own_in, own_at = inside(user_ids, block + own_base, rows)
        oth_in, oth_at = inside(user_ids, block + oth_base, rows)

        def add_up(parts):
            total = parts[0].astype(f32)
            for p in parts[1:]:
                total = total + p.astype(f32)
            return total

        own_id = jnp.where(own_in, own_at, -1)
        oth_id = jnp.where(oth_in, oth_at, -1)
        both = pick_rows(own_id, oth_id, [mine] + own_list, [give] + oth_list)
        picked = scatter_rows(both)
        part_rows = picked[:, :dim]
        last_rows = (part_rows + cross(part_rows)).astype(bf16)
        user_vec = mean([picked[:, dim:], last_rows]).astype(f32)
        table = gather_items(out_item)
        share = count // row_count
        mine_ids = lax.dynamic_slice(triples, (row_idx * share, 0), (share, 3))
        item_in, item_at = inside(mine_ids[:, 1:].T.reshape(-1), col_idx * items, items)
        item_vec = jnp.take(table, item_at, axis=0).astype(f32).reshape(2, share, dim)
        dots = jnp.sum(user_vec[None] * item_vec, axis=2)
        dots = jnp.where(item_in.reshape(2, share), dots, 0.0)
        dots = dots + cross(dots)
        loss_sum = jnp.sum(jax.nn.softplus(dots[1] - dots[0])).reshape(1)
        loss_sum = loss_sum + swap(loss_sum, "row", 1)
        other_sum = swap(loss_sum, "row", 2)
        bpr_loss = ((loss_sum + other_sum) / count).reshape(())

        at = 0
        out_user = None
        for i, n in enumerate(sizes):
            if i == len(sizes) - 1:
                break
            last = (mine[at:at + n] + got[i]).astype(bf16)
            piece = mean([t[at:at + n] for t in own_list] + [last])
            if out_user is None:
                out_user = jnp.pad(piece, ((0, rows - n), (0, 0)))
            else:
                out_user = lax.dynamic_update_slice(out_user, piece, (at, 0))
            at += n
        n = sizes[-1]
        out_user = finish(out_user, mine[rows - n:], got[-1], add_up([t[rows - n:] for t in own_list]))
        return out_user, out_item, bpr_loss

    return jax.shard_map(local_prog, mesh=mesh, in_specs=(P("row", "col"), P(("row", "col"), None), P(("col", "row"), None), P(None, None)), out_specs=(P(("row", "col"), None), P(("col", "row"), None), P()), check_vma=False)
```

```python
import math

import jax
import jax.numpy as jnp
from jax import lax
from jax.experimental import pallas as pl
from jax.experimental.pallas import tpu as pltpu
from jax.sharding import PartitionSpec as P


LAYERS = 3
LAST = LAYERS - 1
TAIL = (8, 7, 1)
FIRST = 2


ROW_BLOCK = 512
LANES = 128


def adj_kernel(base_ref, mask_ref, su_ref, sv_ref, table_ref, *refs):
    adj_ref, part_ref = refs[-2:]

    def rows_of(r, carry):
        at = pl.multiple_of(r * LANES, LANES)
        row_scale = jnp.broadcast_to(su_ref[:, pl.ds(at, LANES)], (LANES, LANES)).T
        for j in range(0, mask_ref.shape[1], LANES):
            m = mask_ref[pl.ds(at, LANES), j:j + LANES].astype(jnp.float32)
            a = m * row_scale * sv_ref[:, j:j + LANES]
            adj_ref[pl.ds(at, LANES), j:j + LANES] = a.astype(jnp.bfloat16)
        return carry

    lax.fori_loop(0, ROW_BLOCK // LANES, rows_of, 0)
    part_ref[...] = jnp.dot(adj_ref[...], table_ref[...], preferred_element_type=jnp.float32)


def make_adj(mask, scale_user, scale_item, table, base, rows, piece, pieces, adj=None):
    items = mask.shape[1]
    dim = table.shape[1]
    blocks = rows // pieces // ROW_BLOCK
    first = piece * blocks
    extra = [] if adj is None else [adj]
    return pl.pallas_call(
        adj_kernel,
        grid_spec=pltpu.PrefetchScalarGridSpec(
            num_scalar_prefetch=1,
            grid=(blocks,),
            in_specs=[
                pl.BlockSpec((ROW_BLOCK, items), lambda i, b: (b[0] + i, 0)),
                pl.BlockSpec((1, ROW_BLOCK), lambda i, b: (0, b[0] + i)),
                pl.BlockSpec((1, items), lambda i, b: (0, 0)),
                pl.BlockSpec((items, dim), lambda i, b: (0, 0)),
            ] + [pl.BlockSpec(memory_space=pl.ANY) for _ in extra],
            out_specs=[
                pl.BlockSpec((ROW_BLOCK, items), lambda i, b: (first + i, 0)),
                pl.BlockSpec((ROW_BLOCK, dim), lambda i, b: (i, 0)),
            ],
        ),
        out_shape=[
            jax.ShapeDtypeStruct((rows, items), jnp.bfloat16),
            jax.ShapeDtypeStruct((rows // pieces, dim), jnp.float32),
        ],
        input_output_aliases={5: 0} if extra else {},
        cost_estimate=pl.CostEstimate(flops=2 * rows // pieces * items * dim, bytes_accessed=rows // pieces * items * 6, transcendentals=0),
    )((base // ROW_BLOCK + first).reshape(1), mask, scale_user.reshape(1, -1), scale_item.reshape(1, -1), table, *extra)


DOT_BLOCK = 2048


def users_kernel(adj_ref, table_ref, part_ref):
    def rows_of(r, carry):
        at = pl.ds(pl.multiple_of(r * ROW_BLOCK, ROW_BLOCK), ROW_BLOCK)
        part_ref[at, :] = jnp.dot(adj_ref[at, :], table_ref[...], preferred_element_type=jnp.float32)
        return carry

    lax.fori_loop(0, adj_ref.shape[0] // ROW_BLOCK, rows_of, 0)


def users_dot(adj, table, first=0, rows=None):
    items = adj.shape[1]
    rows = adj.shape[0] if rows is None else rows
    dim = table.shape[1]
    size = math.gcd(math.gcd(rows, first), DOT_BLOCK)
    at = first // size
    return pl.pallas_call(
        users_kernel,
        grid=(rows // size,),
        in_specs=[pl.BlockSpec((size, items), lambda i: (at + i, 0)), pl.BlockSpec((items, dim), lambda i: (0, 0))],
        out_specs=pl.BlockSpec((size, dim), lambda i: (i, 0)),
        out_shape=jax.ShapeDtypeStruct((rows, dim), jnp.float32),
        cost_estimate=pl.CostEstimate(flops=2 * rows * items * dim, bytes_accessed=rows * items * 2, transcendentals=0),
    )(adj, table)


def items_kernel(start_ref, adj_ref, user_ref, part_ref):
    @pl.when(pl.program_id(0) == 0)
    def _():
        part_ref[...] = start_ref[...]

    def rows_of(r, carry):
        at = pl.ds(pl.multiple_of(r * ROW_BLOCK, ROW_BLOCK), ROW_BLOCK)
        part_ref[...] += lax.dot_general(adj_ref[at, :], user_ref[at, :], (((0,), (0,)), ((), ())), preferred_element_type=jnp.float32)
        return carry

    lax.fori_loop(0, adj_ref.shape[0] // ROW_BLOCK, rows_of, 0)


def items_dot(adj, user, start):
    rows, items = adj.shape
    dim = user.shape[1]
    return pl.pallas_call(
        items_kernel,
        grid=(rows // DOT_BLOCK,),
        in_specs=[
            pl.BlockSpec((items, dim), lambda i: (0, 0)),
            pl.BlockSpec((DOT_BLOCK, items), lambda i: (i, 0)),
            pl.BlockSpec((DOT_BLOCK, dim), lambda i: (i, 0)),
        ],
        out_specs=pl.BlockSpec((items, dim), lambda i: (0, 0)),
        out_shape=jax.ShapeDtypeStruct((items, dim), jnp.float32),
        cost_estimate=pl.CostEstimate(flops=2 * rows * items * dim, bytes_accessed=rows * items * 2, transcendentals=0),
    )(start, adj, user)


PICK_BLOCK = 1024


def pick_kernel(own_id_ref, oth_id_ref, *refs):
    out_ref = refs[-1]
    sides = len(refs) // 2
    step = pl.program_id(0)

    @pl.when(step == 0)
    def _():
        out_ref[...] = jnp.zeros_like(out_ref)

    count = own_id_ref.shape[0]
    at = lax.broadcasted_iota(jnp.int32, (count, PICK_BLOCK), 1) + step * PICK_BLOCK
    dim = refs[0].shape[1]
    for id_ref, tables in ((own_id_ref, refs[:sides]), (oth_id_ref, refs[sides:-1])):
        chosen = jnp.where(id_ref[...] == at, 1.0, 0.0).astype(jnp.bfloat16)
        total = tables[1][...].astype(jnp.float32)
        for t in tables[2:]:
            total = total + t[...].astype(jnp.float32)
        for place, value in ((0, tables[0][...]), (dim, total)):
            for _ in range(3):
                part = value.astype(jnp.bfloat16)
                out_ref[:, place:place + dim] += jnp.dot(chosen, part, preferred_element_type=jnp.float32)
                value = value - part.astype(jnp.float32)


def pick_rows(own_id, oth_id, own_tables, oth_tables):
    rows, dim = own_tables[0].shape
    count = own_id.shape[0]
    ids = pl.BlockSpec((count, 1), lambda i: (0, 0))
    block = pl.BlockSpec((PICK_BLOCK, dim), lambda i: (i, 0))
    return pl.pallas_call(
        pick_kernel,
        grid=(rows // PICK_BLOCK,),
        in_specs=[ids, ids] + [block] * (len(own_tables) + len(oth_tables)),
        out_specs=pl.BlockSpec((count, 2 * dim), lambda i: (0, 0)),
        out_shape=jax.ShapeDtypeStruct((count, 2 * dim), jnp.float32),
        cost_estimate=pl.CostEstimate(flops=24 * count * rows * dim, bytes_accessed=20 * rows * dim, transcendentals=0),
    )(own_id.reshape(count, 1), oth_id.reshape(count, 1), *own_tables, *oth_tables)


def finish_kernel(done_ref, mine_ref, got_ref, base_ref, out_ref, piece_ref, sem):
    last = (mine_ref[...] + got_ref[...]).astype(jnp.bfloat16).astype(jnp.float32)
    piece_ref[...] = ((base_ref[...] + last) / (LAYERS + 1)).astype(jnp.bfloat16)
    n = piece_ref.shape[0]
    copy = pltpu.make_async_copy(piece_ref, out_ref.at[pl.ds(out_ref.shape[0] - n, n)], sem)
    copy.start()
    copy.wait()


def finish(done, mine, got, base):
    rows, dim = done.shape
    n = got.shape[0]
    vmem = pl.BlockSpec(memory_space=pltpu.VMEM)
    return pl.pallas_call(
        finish_kernel,
        in_specs=[pl.BlockSpec(memory_space=pltpu.HBM), vmem, vmem, vmem],
        out_specs=pl.BlockSpec(memory_space=pltpu.HBM),
        out_shape=jax.ShapeDtypeStruct((rows, dim), jnp.bfloat16),
        input_output_aliases={0: 0},
        scratch_shapes=[pltpu.VMEM((n, dim), jnp.bfloat16), pltpu.SemaphoreType.DMA],
        cost_estimate=pl.CostEstimate(flops=8 * n * dim, bytes_accessed=16 * n * dim, transcendentals=0),
    )(done, mine, got, base)


def solution(mesh):
    row_count = mesh.shape["row"]
    col_count = mesh.shape["col"]
    f32 = jnp.float32
    bf16 = jnp.bfloat16

    def swap(value, axis, bit):
        pairs = [(i, i ^ bit) for i in range(mesh.shape[axis])]
        return lax.ppermute(value, axis, pairs)

    def cross(value):
        pairs = [(i, i ^ row_count ^ 2) for i in range(row_count * col_count)]
        value = lax.ppermute(value, ("col", "row"), pairs)
        return swap(value, "row", 2)

    def local_prog(mask_blk, user_shard, item_shard, triples):
        row_idx = lax.axis_index("row")
        col_idx = lax.axis_index("col")
        x_idx = row_idx >> 1
        core_idx = row_idx & 1
        rows = user_shard.shape[0]
        items = mask_blk.shape[1]
        dim = user_shard.shape[1]
        own_base = col_idx * rows
        oth_base = (1 - col_idx) * rows
        count = triples.shape[0]

        def gather_items(shard):
            other = swap(shard, "row", 2)
            first = x_idx == 0
            pair = jnp.stack([jnp.where(first, shard, other), jnp.where(first, other, shard)], axis=0)
            peer = swap(pair, "row", 1)
            first = core_idx == 0
            panel = jnp.stack([jnp.where(first, pair, peer), jnp.where(first, peer, pair)], axis=1)
            return panel.reshape(items, dim)

        def scatter_rows(part):
            blocks = part.reshape(2, 2, part.shape[0] // 4, part.shape[1])
            keep = lax.dynamic_index_in_dim(blocks, core_idx, 1, keepdims=False)
            give = lax.dynamic_index_in_dim(blocks, 1 - core_idx, 1, keepdims=False)
            half = keep + swap(give, "row", 1)
            keep = lax.dynamic_index_in_dim(half, x_idx, 0, keepdims=False)
            give = lax.dynamic_index_in_dim(half, 1 - x_idx, 0, keepdims=False)
            return keep + swap(give, "row", 2)

        oth = swap(user_shard, "col", 1)
        panel = gather_items(item_shard)

        deg_user = jnp.sum(mask_blk, axis=1)
        deg_item = jnp.sum(mask_blk, axis=0)
        deg_user = jnp.maximum(deg_user + cross(deg_user), 1)
        deg_item = deg_item + swap(deg_item, "row", 1)
        deg_item = jnp.maximum(deg_item + swap(deg_item, "row", 2), 1)
        scale_user = lax.rsqrt(deg_user.astype(f32))
        scale_item = lax.rsqrt(deg_item.astype(f32))

        adj_oth = None
        give0 = []
        for i in range(FIRST):
            adj_oth, piece = make_adj(mask_blk, scale_user, scale_item, panel, oth_base, rows, i, FIRST, adj_oth)
            give0.append(piece)
        adj_own, mine0 = make_adj(mask_blk, scale_user, scale_item, panel, own_base, rows, 0, 1)

        own = user_shard
        item = item_shard
        own_list = [own]
        oth_list = [oth]
        item_list = [item]
        sizes = [rows * t // sum(TAIL) for t in TAIL]
        for k in range(LAYERS):
            if k == 0:
                got = [jnp.concatenate([swap(g, "col", 1) for g in give0], axis=0)]
            elif k < LAST:
                give = users_dot(adj_oth, panel)
                got = [swap(give, "col", 1)]
            else:
                got, give, at = [], [], 0
                for n in sizes:
                    give.append(users_dot(adj_oth, panel, at, n))
                    got.append(swap(give[-1], "col", 1))
                    at += n
                oth, _ = lax.optimization_barrier((oth, give[-1]))
                give = jnp.concatenate(give, axis=0)
            mine = mine0 if k == 0 else users_dot(adj_own, panel)
            part = items_dot(adj_own, own, jnp.zeros((items, dim), f32))
            part = items_dot(adj_oth, oth, part)
            item = scatter_rows(part).astype(bf16)
            item_list.append(item)
            if k < LAST:
                own = (mine + got[0]).astype(bf16)
                own_list.append(own)
                oth = swap(own, "col", 1)
                oth_list.append(oth)
                panel = gather_items(item)

        def mean(parts):
            total = parts[0].astype(f32)
            for p in parts[1:]:
                total = total + p.astype(f32)
            return (total / (LAYERS + 1)).astype(bf16)

        out_item = mean(item_list)

        def inside(ids, base, n):
            local = ids - base
            return (local >= 0) & (local < n), jnp.clip(local, 0, n - 1)

        user_ids = triples[:, 0]
        block = row_idx * col_count * rows
        own_in, own_at = inside(user_ids, block + own_base, rows)
        oth_in, oth_at = inside(user_ids, block + oth_base, rows)

        def add_up(parts):
            total = parts[0].astype(f32)
            for p in parts[1:]:
                total = total + p.astype(f32)
            return total

        own_id = jnp.where(own_in, own_at, -1)
        oth_id = jnp.where(oth_in, oth_at, -1)
        both = pick_rows(own_id, oth_id, [mine] + own_list, [give] + oth_list)
        picked = scatter_rows(both)
        part_rows = picked[:, :dim]
        last_rows = (part_rows + cross(part_rows)).astype(bf16)
        user_vec = mean([picked[:, dim:], last_rows]).astype(f32)
        table = gather_items(out_item)
        share = count // row_count
        mine_ids = lax.dynamic_slice(triples, (row_idx * share, 0), (share, 3))
        item_in, item_at = inside(mine_ids[:, 1:].T.reshape(-1), col_idx * items, items)
        item_vec = jnp.take(table, item_at, axis=0).astype(f32).reshape(2, share, dim)
        dots = jnp.sum(user_vec[None] * item_vec, axis=2)
        dots = jnp.where(item_in.reshape(2, share), dots, 0.0)
        dots = dots + cross(dots)
        loss_sum = jnp.sum(jax.nn.softplus(dots[1] - dots[0])).reshape(1)
        loss_sum = loss_sum + swap(loss_sum, "row", 1)
        other_sum = swap(loss_sum, "row", 2)
        bpr_loss = ((loss_sum + other_sum) / count).reshape(())

        at = 0
        out_user = None
        for i, n in enumerate(sizes):
            if i == len(sizes) - 1:
                break
            last = (mine[at:at + n] + got[i]).astype(bf16)
            piece = mean([t[at:at + n] for t in own_list] + [last])
            if out_user is None:
                out_user = jnp.pad(piece, ((0, rows - n), (0, 0)))
            else:
                out_user = lax.dynamic_update_slice(out_user, piece, (at, 0))
            at += n
        n = sizes[-1]
        out_user = finish(out_user, mine[rows - n:], got[-1], add_up([t[rows - n:] for t in own_list]))
        return out_user, out_item, bpr_loss

    return jax.shard_map(local_prog, mesh=mesh, in_specs=(P("row", "col"), P(("row", "col"), None), P(("col", "row"), None), P(None, None)), out_specs=(P(("row", "col"), None), P(("col", "row"), None), P()), check_vma=False)
```

```python
import math

import jax
import jax.numpy as jnp
from jax import lax
from jax.experimental import pallas as pl
from jax.experimental.pallas import tpu as pltpu
from jax.sharding import PartitionSpec as P


LAYERS = 3
LAST = LAYERS - 1
TAIL = (16, 14, 1, 1)
FIRST = 2


ROW_BLOCK = 512
ADJ_BLOCK = 1024
LANES = 128


def adj_kernel(base_ref, mask_ref, su_ref, sv_ref, table_ref, *refs):
    adj_ref, part_ref = refs[-2:]

    def rows_of(r, carry):
        at = pl.multiple_of(r * LANES, LANES)
        row_scale = jnp.broadcast_to(su_ref[:, pl.ds(at, LANES)], (LANES, LANES)).T
        for j in range(0, mask_ref.shape[1], LANES):
            m = mask_ref[pl.ds(at, LANES), j:j + LANES].astype(jnp.float32)
            a = m * row_scale * sv_ref[:, j:j + LANES]
            adj_ref[pl.ds(at, LANES), j:j + LANES] = a.astype(jnp.bfloat16)
        return carry

    lax.fori_loop(0, ADJ_BLOCK // LANES, rows_of, 0)
    users_kernel(adj_ref, table_ref, part_ref)


def make_adj(mask, scale_user, scale_item, table, base, rows, piece, pieces, adj=None):
    items = mask.shape[1]
    dim = table.shape[1]
    blocks = rows // pieces // ADJ_BLOCK
    first = piece * blocks
    extra = [] if adj is None else [adj]
    return pl.pallas_call(
        adj_kernel,
        grid_spec=pltpu.PrefetchScalarGridSpec(
            num_scalar_prefetch=1,
            grid=(blocks,),
            in_specs=[
                pl.BlockSpec((ADJ_BLOCK, items), lambda i, b: (b[0] + i, 0)),
                pl.BlockSpec((1, ADJ_BLOCK), lambda i, b: (0, b[0] + i)),
                pl.BlockSpec((1, items), lambda i, b: (0, 0)),
                pl.BlockSpec((items, dim), lambda i, b: (0, 0)),
            ] + [pl.BlockSpec(memory_space=pl.ANY) for _ in extra],
            out_specs=[
                pl.BlockSpec((ADJ_BLOCK, items), lambda i, b: (first + i, 0)),
                pl.BlockSpec((ADJ_BLOCK, dim), lambda i, b: (i, 0)),
            ],
        ),
        out_shape=[
            jax.ShapeDtypeStruct((rows, items), jnp.bfloat16),
            jax.ShapeDtypeStruct((rows // pieces, dim), jnp.float32),
        ],
        input_output_aliases={5: 0} if extra else {},
        cost_estimate=pl.CostEstimate(flops=2 * rows // pieces * items * dim, bytes_accessed=rows // pieces * items * 6, transcendentals=0),
    )((base // ADJ_BLOCK + first).reshape(1), mask, scale_user.reshape(1, -1), scale_item.reshape(1, -1), table, *extra)


DOT_BLOCK = 2048


def users_kernel(adj_ref, table_ref, part_ref):
    inner = min(adj_ref.shape[0], ROW_BLOCK)

    def rows_of(r, carry):
        at = pl.ds(pl.multiple_of(r * inner, inner), inner)
        part_ref[at, :] = jnp.dot(adj_ref[at, :], table_ref[...], preferred_element_type=jnp.float32)
        return carry

    lax.fori_loop(0, adj_ref.shape[0] // inner, rows_of, 0)


def users_dot(adj, table, first=0, rows=None):
    items = adj.shape[1]
    rows = adj.shape[0] if rows is None else rows
    dim = table.shape[1]
    size = math.gcd(math.gcd(rows, first), DOT_BLOCK)
    at = first // size
    return pl.pallas_call(
        users_kernel,
        grid=(rows // size,),
        in_specs=[pl.BlockSpec((size, items), lambda i: (at + i, 0)), pl.BlockSpec((items, dim), lambda i: (0, 0))],
        out_specs=pl.BlockSpec((size, dim), lambda i: (i, 0)),
        out_shape=jax.ShapeDtypeStruct((rows, dim), jnp.float32),
        cost_estimate=pl.CostEstimate(flops=2 * rows * items * dim, bytes_accessed=rows * items * 2, transcendentals=0),
    )(adj, table)


def items_kernel(start_ref, adj_ref, user_ref, part_ref):
    @pl.when(pl.program_id(0) == 0)
    def _():
        part_ref[...] = start_ref[...]

    def rows_of(r, carry):
        at = pl.ds(pl.multiple_of(r * ROW_BLOCK, ROW_BLOCK), ROW_BLOCK)
        part_ref[...] += lax.dot_general(adj_ref[at, :], user_ref[at, :], (((0,), (0,)), ((), ())), preferred_element_type=jnp.float32)
        return carry

    lax.fori_loop(0, adj_ref.shape[0] // ROW_BLOCK, rows_of, 0)


def items_dot(adj, user, start):
    rows, items = adj.shape
    dim = user.shape[1]
    return pl.pallas_call(
        items_kernel,
        grid=(rows // DOT_BLOCK,),
        in_specs=[
            pl.BlockSpec((items, dim), lambda i: (0, 0)),
            pl.BlockSpec((DOT_BLOCK, items), lambda i: (i, 0)),
            pl.BlockSpec((DOT_BLOCK, dim), lambda i: (i, 0)),
        ],
        out_specs=pl.BlockSpec((items, dim), lambda i: (0, 0)),
        out_shape=jax.ShapeDtypeStruct((items, dim), jnp.float32),
        cost_estimate=pl.CostEstimate(flops=2 * rows * items * dim, bytes_accessed=rows * items * 2, transcendentals=0),
    )(start, adj, user)


PICK_BLOCK = 1024


def pick_kernel(own_id_ref, oth_id_ref, *refs):
    out_ref = refs[-1]
    sides = len(refs) // 2
    step = pl.program_id(0)

    @pl.when(step == 0)
    def _():
        out_ref[...] = jnp.zeros_like(out_ref)

    count = own_id_ref.shape[0]
    at = lax.broadcasted_iota(jnp.int32, (count, PICK_BLOCK), 1) + step * PICK_BLOCK
    dim = refs[0].shape[1]
    for id_ref, tables in ((own_id_ref, refs[:sides]), (oth_id_ref, refs[sides:-1])):
        chosen = jnp.where(id_ref[...] == at, 1.0, 0.0).astype(jnp.bfloat16)
        total = tables[1][...].astype(jnp.float32)
        for t in tables[2:]:
            total = total + t[...].astype(jnp.float32)
        for place, value in ((0, tables[0][...]), (dim, total)):
            for _ in range(3):
                part = value.astype(jnp.bfloat16)
                out_ref[:, place:place + dim] += jnp.dot(chosen, part, preferred_element_type=jnp.float32)
                value = value - part.astype(jnp.float32)


def pick_rows(own_id, oth_id, own_tables, oth_tables):
    rows, dim = own_tables[0].shape
    count = own_id.shape[0]
    ids = pl.BlockSpec((count, 1), lambda i: (0, 0))
    block = pl.BlockSpec((PICK_BLOCK, dim), lambda i: (i, 0))
    return pl.pallas_call(
        pick_kernel,
        grid=(rows // PICK_BLOCK,),
        in_specs=[ids, ids] + [block] * (len(own_tables) + len(oth_tables)),
        out_specs=pl.BlockSpec((count, 2 * dim), lambda i: (0, 0)),
        out_shape=jax.ShapeDtypeStruct((count, 2 * dim), jnp.float32),
        cost_estimate=pl.CostEstimate(flops=24 * count * rows * dim, bytes_accessed=20 * rows * dim, transcendentals=0),
    )(own_id.reshape(count, 1), oth_id.reshape(count, 1), *own_tables, *oth_tables)


def finish_kernel(done_ref, mine_ref, got_ref, base_ref, out_ref, piece_ref, sem):
    last = (mine_ref[...] + got_ref[...]).astype(jnp.bfloat16).astype(jnp.float32)
    piece_ref[...] = ((base_ref[...] + last) / (LAYERS + 1)).astype(jnp.bfloat16)
    n = piece_ref.shape[0]
    copy = pltpu.make_async_copy(piece_ref, out_ref.at[pl.ds(out_ref.shape[0] - n, n)], sem)
    copy.start()
    copy.wait()


def finish(done, mine, got, base):
    rows, dim = done.shape
    n = got.shape[0]
    vmem = pl.BlockSpec(memory_space=pltpu.VMEM)
    return pl.pallas_call(
        finish_kernel,
        in_specs=[pl.BlockSpec(memory_space=pltpu.HBM), vmem, vmem, vmem],
        out_specs=pl.BlockSpec(memory_space=pltpu.HBM),
        out_shape=jax.ShapeDtypeStruct((rows, dim), jnp.bfloat16),
        input_output_aliases={0: 0},
        scratch_shapes=[pltpu.VMEM((n, dim), jnp.bfloat16), pltpu.SemaphoreType.DMA],
        compiler_params=pltpu.CompilerParams(vmem_limit_bytes=4 * 2**20),
        cost_estimate=pl.CostEstimate(flops=8 * n * dim, bytes_accessed=16 * n * dim, transcendentals=0),
    )(done, mine, got, base)


def solution(mesh):
    row_count = mesh.shape["row"]
    col_count = mesh.shape["col"]
    f32 = jnp.float32
    bf16 = jnp.bfloat16

    def swap(value, axis, bit):
        pairs = [(i, i ^ bit) for i in range(mesh.shape[axis])]
        return lax.ppermute(value, axis, pairs)

    def cross(value):
        pairs = [(i, i ^ row_count ^ 2) for i in range(row_count * col_count)]
        value = lax.ppermute(value, ("col", "row"), pairs)
        return swap(value, "row", 2)

    def local_prog(mask_blk, user_shard, item_shard, triples):
        row_idx = lax.axis_index("row")
        col_idx = lax.axis_index("col")
        x_idx = row_idx >> 1
        core_idx = row_idx & 1
        rows = user_shard.shape[0]
        items = mask_blk.shape[1]
        dim = user_shard.shape[1]
        own_base = col_idx * rows
        oth_base = (1 - col_idx) * rows
        count = triples.shape[0]

        def gather_items(shard):
            other = swap(shard, "row", 2)
            first = x_idx == 0
            pair = jnp.stack([jnp.where(first, shard, other), jnp.where(first, other, shard)], axis=0)
            peer = swap(pair, "row", 1)
            first = core_idx == 0
            panel = jnp.stack([jnp.where(first, pair, peer), jnp.where(first, peer, pair)], axis=1)
            return panel.reshape(items, dim)

        def scatter_rows(part):
            blocks = part.reshape(2, 2, part.shape[0] // 4, part.shape[1])
            keep = lax.dynamic_index_in_dim(blocks, core_idx, 1, keepdims=False)
            give = lax.dynamic_index_in_dim(blocks, 1 - core_idx, 1, keepdims=False)
            half = keep + swap(give, "row", 1)
            keep = lax.dynamic_index_in_dim(half, x_idx, 0, keepdims=False)
            give = lax.dynamic_index_in_dim(half, 1 - x_idx, 0, keepdims=False)
            return keep + swap(give, "row", 2)

        oth = swap(user_shard, "col", 1)
        panel = gather_items(item_shard)

        deg_user = jnp.sum(mask_blk, axis=1)
        deg_item = jnp.sum(mask_blk, axis=0)
        deg_user = jnp.maximum(deg_user + cross(deg_user), 1)
        deg_item = deg_item + swap(deg_item, "row", 1)
        deg_item = jnp.maximum(deg_item + swap(deg_item, "row", 2), 1)
        scale_user = lax.rsqrt(deg_user.astype(f32))
        scale_item = lax.rsqrt(deg_item.astype(f32))

        adj_oth = None
        give0 = []
        for i in range(FIRST):
            adj_oth, piece = make_adj(mask_blk, scale_user, scale_item, panel, oth_base, rows, i, FIRST, adj_oth)
            give0.append(piece)
        adj_own, mine0 = make_adj(mask_blk, scale_user, scale_item, panel, own_base, rows, 0, 1)

        own = user_shard
        item = item_shard
        own_list = [own]
        oth_list = [oth]
        item_list = [item]
        sizes = [rows * t // sum(TAIL) for t in TAIL]
        for k in range(LAYERS):
            if k == 0:
                got = [jnp.concatenate([swap(g, "col", 1) for g in give0], axis=0)]
            elif k < LAST:
                give = users_dot(adj_oth, panel)
                got = [swap(give, "col", 1)]
            else:
                got, give, at = [], [], 0
                for n in sizes:
                    give.append(users_dot(adj_oth, panel, at, n))
                    got.append(swap(give[-1], "col", 1))
                    at += n
                oth, _ = lax.optimization_barrier((oth, give[-1]))
                give = jnp.concatenate(give, axis=0)
            mine = mine0 if k == 0 else users_dot(adj_own, panel)
            part = items_dot(adj_own, own, jnp.zeros((items, dim), f32))
            part = items_dot(adj_oth, oth, part)
            item = scatter_rows(part).astype(bf16)
            item_list.append(item)
            if k < LAST:
                own = (mine + got[0]).astype(bf16)
                own_list.append(own)
                oth = swap(own, "col", 1)
                oth_list.append(oth)
                panel = gather_items(item)

        def mean(parts):
            total = parts[0].astype(f32)
            for p in parts[1:]:
                total = total + p.astype(f32)
            return (total / (LAYERS + 1)).astype(bf16)

        out_item = mean(item_list)

        def inside(ids, base, n):
            local = ids - base
            return (local >= 0) & (local < n), jnp.clip(local, 0, n - 1)

        user_ids = triples[:, 0]
        block = row_idx * col_count * rows
        own_in, own_at = inside(user_ids, block + own_base, rows)
        oth_in, oth_at = inside(user_ids, block + oth_base, rows)

        def add_up(parts):
            total = parts[0].astype(f32)
            for p in parts[1:]:
                total = total + p.astype(f32)
            return total

        own_id = jnp.where(own_in, own_at, -1)
        oth_id = jnp.where(oth_in, oth_at, -1)
        both = pick_rows(own_id, oth_id, [mine] + own_list, [give] + oth_list)
        picked = scatter_rows(both)
        part_rows = picked[:, :dim]
        last_rows = (part_rows + cross(part_rows)).astype(bf16)
        user_vec = mean([picked[:, dim:], last_rows]).astype(f32)
        table = gather_items(out_item)
        share = count // row_count
        mine_ids = lax.dynamic_slice(triples, (row_idx * share, 0), (share, 3))
        item_in, item_at = inside(mine_ids[:, 1:].T.reshape(-1), col_idx * items, items)
        item_vec = jnp.take(table, item_at, axis=0).astype(f32).reshape(2, share, dim)
        dots = jnp.sum(user_vec[None] * item_vec, axis=2)
        dots = jnp.where(item_in.reshape(2, share), dots, 0.0)
        dots = dots + cross(dots)
        loss_sum = jnp.sum(jax.nn.softplus(dots[1] - dots[0])).reshape(1)
        loss_sum = loss_sum + swap(loss_sum, "row", 1)
        other_sum = swap(loss_sum, "row", 2)
        bpr_loss = ((loss_sum + other_sum) / count).reshape(())

        at = 0
        out_user = None
        for i, n in enumerate(sizes):
            if i == len(sizes) - 1:
                break
            last = (mine[at:at + n] + got[i]).astype(bf16)
            piece = mean([t[at:at + n] for t in own_list] + [last])
            if out_user is None:
                out_user = jnp.pad(piece, ((0, rows - n), (0, 0)))
            else:
                out_user = lax.dynamic_update_slice(out_user, piece, (at, 0))
            at += n
        n = sizes[-1]
        out_user = finish(out_user, mine[rows - n:], got[-1], add_up([t[rows - n:] for t in own_list]))
        return out_user, out_item, bpr_loss

    return jax.shard_map(local_prog, mesh=mesh, in_specs=(P("row", "col"), P(("row", "col"), None), P(("col", "row"), None), P(None, None)), out_specs=(P(("row", "col"), None), P(("col", "row"), None), P()), check_vma=False)
```

```python
import math

import jax
import jax.numpy as jnp
from jax import lax
from jax.experimental import pallas as pl
from jax.experimental.pallas import tpu as pltpu
from jax.sharding import PartitionSpec as P


LAYERS = 3
LAST = LAYERS - 1
TAIL = (16, 14, 1, 1)
FIRST = 2


ROW_BLOCK = 512
ADJ_BLOCK = 1024
LANES = 128


def adj_kernel(base_ref, mask_ref, su_ref, sv_ref, table_ref, *refs):
    adj_ref, part_ref = refs[-2:]

    def rows_of(r, carry):
        at = pl.multiple_of(r * LANES, LANES)
        row_scale = jnp.broadcast_to(su_ref[:, pl.ds(at, LANES)], (LANES, LANES)).T
        for j in range(0, mask_ref.shape[1], LANES):
            m = mask_ref[pl.ds(at, LANES), j:j + LANES].astype(jnp.float32)
            a = m * row_scale * sv_ref[:, j:j + LANES]
            adj_ref[pl.ds(at, LANES), j:j + LANES] = a.astype(jnp.bfloat16)
        return carry

    lax.fori_loop(0, ADJ_BLOCK // LANES, rows_of, 0)
    users_kernel(adj_ref, table_ref, part_ref)


def make_adj(mask, scale_user, scale_item, table, base, rows, piece, pieces, adj=None):
    items = mask.shape[1]
    dim = table.shape[1]
    blocks = rows // pieces // ADJ_BLOCK
    first = piece * blocks
    extra = [] if adj is None else [adj]
    return pl.pallas_call(
        adj_kernel,
        grid_spec=pltpu.PrefetchScalarGridSpec(
            num_scalar_prefetch=1,
            grid=(blocks,),
            in_specs=[
                pl.BlockSpec((ADJ_BLOCK, items), lambda i, b: (b[0] + i, 0)),
                pl.BlockSpec((1, ADJ_BLOCK), lambda i, b: (0, b[0] + i)),
                pl.BlockSpec((1, items), lambda i, b: (0, 0)),
                pl.BlockSpec((items, dim), lambda i, b: (0, 0)),
            ] + [pl.BlockSpec(memory_space=pl.ANY) for _ in extra],
            out_specs=[
                pl.BlockSpec((ADJ_BLOCK, items), lambda i, b: (first + i, 0)),
                pl.BlockSpec((ADJ_BLOCK, dim), lambda i, b: (i, 0)),
            ],
        ),
        out_shape=[
            jax.ShapeDtypeStruct((rows, items), jnp.bfloat16),
            jax.ShapeDtypeStruct((rows // pieces, dim), jnp.float32),
        ],
        input_output_aliases={5: 0} if extra else {},
        compiler_params=pltpu.CompilerParams(vmem_limit_bytes=34 * 2**20),
        cost_estimate=pl.CostEstimate(flops=2 * rows // pieces * items * dim, bytes_accessed=rows // pieces * items * 6, transcendentals=0),
    )((base // ADJ_BLOCK + first).reshape(1), mask, scale_user.reshape(1, -1), scale_item.reshape(1, -1), table, *extra)


DOT_BLOCK = 2048


def users_kernel(adj_ref, table_ref, part_ref):
    inner = min(adj_ref.shape[0], ROW_BLOCK)

    def rows_of(r, carry):
        at = pl.ds(pl.multiple_of(r * inner, inner), inner)
        part_ref[at, :] = jnp.dot(adj_ref[at, :], table_ref[...], preferred_element_type=jnp.float32)
        return carry

    lax.fori_loop(0, adj_ref.shape[0] // inner, rows_of, 0)


def users_dot(adj, table, first=0, rows=None):
    items = adj.shape[1]
    rows = adj.shape[0] if rows is None else rows
    dim = table.shape[1]
    size = math.gcd(math.gcd(rows, first), DOT_BLOCK)
    at = first // size
    return pl.pallas_call(
        users_kernel,
        grid=(rows // size,),
        in_specs=[pl.BlockSpec((size, items), lambda i: (at + i, 0)), pl.BlockSpec((items, dim), lambda i: (0, 0))],
        out_specs=pl.BlockSpec((size, dim), lambda i: (i, 0)),
        out_shape=jax.ShapeDtypeStruct((rows, dim), jnp.float32),
        compiler_params=pltpu.CompilerParams(vmem_limit_bytes=28 * 2**20),
        cost_estimate=pl.CostEstimate(flops=2 * rows * items * dim, bytes_accessed=rows * items * 2, transcendentals=0),
    )(adj, table)


def items_kernel(start_ref, adj_ref, user_ref, part_ref):
    @pl.when(pl.program_id(0) == 0)
    def _():
        part_ref[...] = start_ref[...]

    def rows_of(r, carry):
        at = pl.ds(pl.multiple_of(r * ROW_BLOCK, ROW_BLOCK), ROW_BLOCK)
        part_ref[...] += lax.dot_general(adj_ref[at, :], user_ref[at, :], (((0,), (0,)), ((), ())), preferred_element_type=jnp.float32)
        return carry

    lax.fori_loop(0, adj_ref.shape[0] // ROW_BLOCK, rows_of, 0)


def items_dot(adj, user, start):
    rows, items = adj.shape
    dim = user.shape[1]
    return pl.pallas_call(
        items_kernel,
        grid=(rows // DOT_BLOCK,),
        in_specs=[
            pl.BlockSpec((items, dim), lambda i: (0, 0)),
            pl.BlockSpec((DOT_BLOCK, items), lambda i: (i, 0)),
            pl.BlockSpec((DOT_BLOCK, dim), lambda i: (i, 0)),
        ],
        out_specs=pl.BlockSpec((items, dim), lambda i: (0, 0)),
        out_shape=jax.ShapeDtypeStruct((items, dim), jnp.float32),
        compiler_params=pltpu.CompilerParams(vmem_limit_bytes=34 * 2**20),
        cost_estimate=pl.CostEstimate(flops=2 * rows * items * dim, bytes_accessed=rows * items * 2, transcendentals=0),
    )(start, adj, user)


PICK_BLOCK = 1024
BF16_MAX = float(jnp.finfo(jnp.bfloat16).max)


def pick_kernel(own_id_ref, oth_id_ref, *refs):
    out_ref = refs[-1]
    sides = len(refs) // 2
    step = pl.program_id(0)

    @pl.when(step == 0)
    def _():
        out_ref[...] = jnp.zeros_like(out_ref)

    count = own_id_ref.shape[0]
    at = lax.broadcasted_iota(jnp.int32, (count, PICK_BLOCK), 1) + step * PICK_BLOCK
    dim = refs[0].shape[1]
    for id_ref, tables in ((own_id_ref, refs[:sides]), (oth_id_ref, refs[sides:-1])):
        chosen = jnp.where(id_ref[...] == at, 1.0, 0.0).astype(jnp.bfloat16)
        total = tables[1][...].astype(jnp.float32)
        for t in tables[2:]:
            total = total + t[...].astype(jnp.float32)
        for place, value in ((0, tables[0][...]), (dim, total)):
            for _ in range(3):
                part = jnp.clip(value, -BF16_MAX, BF16_MAX).astype(jnp.bfloat16)
                out_ref[:, place:place + dim] += jnp.dot(chosen, part, preferred_element_type=jnp.float32)
                value = value - part.astype(jnp.float32)


def pick_rows(own_id, oth_id, own_tables, oth_tables):
    rows, dim = own_tables[0].shape
    count = own_id.shape[0]
    ids = pl.BlockSpec((count, 1), lambda i: (0, 0))
    block = pl.BlockSpec((PICK_BLOCK, dim), lambda i: (i, 0))
    return pl.pallas_call(
        pick_kernel,
        grid=(rows // PICK_BLOCK,),
        in_specs=[ids, ids] + [block] * (len(own_tables) + len(oth_tables)),
        out_specs=pl.BlockSpec((count, 2 * dim), lambda i: (0, 0)),
        out_shape=jax.ShapeDtypeStruct((count, 2 * dim), jnp.float32),
        compiler_params=pltpu.CompilerParams(vmem_limit_bytes=28 * 2**20),
        cost_estimate=pl.CostEstimate(flops=24 * count * rows * dim, bytes_accessed=20 * rows * dim, transcendentals=0),
    )(own_id.reshape(count, 1), oth_id.reshape(count, 1), *own_tables, *oth_tables)


def finish_kernel(done_ref, mine_ref, got_ref, base_ref, out_ref, piece_ref, sem):
    last = (mine_ref[...] + got_ref[...]).astype(jnp.bfloat16).astype(jnp.float32)
    piece_ref[...] = ((base_ref[...] + last) / (LAYERS + 1)).astype(jnp.bfloat16)
    n = piece_ref.shape[0]
    copy = pltpu.make_async_copy(piece_ref, out_ref.at[pl.ds(out_ref.shape[0] - n, n)], sem)
    copy.start()
    copy.wait()


def finish(done, mine, got, base):
    rows, dim = done.shape
    n = got.shape[0]
    vmem = pl.BlockSpec(memory_space=pltpu.VMEM)
    return pl.pallas_call(
        finish_kernel,
        in_specs=[pl.BlockSpec(memory_space=pltpu.HBM), vmem, vmem, vmem],
        out_specs=pl.BlockSpec(memory_space=pltpu.HBM),
        out_shape=jax.ShapeDtypeStruct((rows, dim), jnp.bfloat16),
        input_output_aliases={0: 0},
        scratch_shapes=[pltpu.VMEM((n, dim), jnp.bfloat16), pltpu.SemaphoreType.DMA],
        compiler_params=pltpu.CompilerParams(vmem_limit_bytes=4 * 2**20),
        cost_estimate=pl.CostEstimate(flops=8 * n * dim, bytes_accessed=16 * n * dim, transcendentals=0),
    )(done, mine, got, base)


def solution(mesh):
    row_count = mesh.shape["row"]
    col_count = mesh.shape["col"]
    f32 = jnp.float32
    bf16 = jnp.bfloat16

    def swap(value, axis, bit):
        pairs = [(i, i ^ bit) for i in range(mesh.shape[axis])]
        return lax.ppermute(value, axis, pairs)

    def cross(value):
        pairs = [(i, i ^ row_count ^ 2) for i in range(row_count * col_count)]
        value = lax.ppermute(value, ("col", "row"), pairs)
        return swap(value, "row", 2)

    def local_prog(mask_blk, user_shard, item_shard, triples):
        row_idx = lax.axis_index("row")
        col_idx = lax.axis_index("col")
        x_idx = row_idx >> 1
        core_idx = row_idx & 1
        rows = user_shard.shape[0]
        items = mask_blk.shape[1]
        dim = user_shard.shape[1]
        own_base = col_idx * rows
        oth_base = (1 - col_idx) * rows
        count = triples.shape[0]

        def gather_items(shard):
            other = swap(shard, "row", 2)
            first = x_idx == 0
            pair = jnp.stack([jnp.where(first, shard, other), jnp.where(first, other, shard)], axis=0)
            peer = swap(pair, "row", 1)
            first = core_idx == 0
            panel = jnp.stack([jnp.where(first, pair, peer), jnp.where(first, peer, pair)], axis=1)
            return panel.reshape(items, dim)

        def scatter_rows(part):
            blocks = part.reshape(2, 2, part.shape[0] // 4, part.shape[1])
            keep = lax.dynamic_index_in_dim(blocks, core_idx, 1, keepdims=False)
            give = lax.dynamic_index_in_dim(blocks, 1 - core_idx, 1, keepdims=False)
            half = keep + swap(give, "row", 1)
            keep = lax.dynamic_index_in_dim(half, x_idx, 0, keepdims=False)
            give = lax.dynamic_index_in_dim(half, 1 - x_idx, 0, keepdims=False)
            return keep + swap(give, "row", 2)

        oth = swap(user_shard, "col", 1)
        panel = gather_items(item_shard)

        deg_user = jnp.sum(mask_blk, axis=1)
        deg_item = jnp.sum(mask_blk, axis=0)
        deg_user = jnp.maximum(deg_user + cross(deg_user), 1)
        deg_item = deg_item + swap(deg_item, "row", 1)
        deg_item = jnp.maximum(deg_item + swap(deg_item, "row", 2), 1)
        scale_user = lax.rsqrt(deg_user.astype(f32))
        scale_item = lax.rsqrt(deg_item.astype(f32))

        adj_oth = None
        give0 = []
        for i in range(FIRST):
            adj_oth, piece = make_adj(mask_blk, scale_user, scale_item, panel, oth_base, rows, i, FIRST, adj_oth)
            give0.append(piece)
        adj_own, mine0 = make_adj(mask_blk, scale_user, scale_item, panel, own_base, rows, 0, 1)

        own = user_shard
        item = item_shard
        own_list = [own]
        oth_list = [oth]
        item_list = [item]
        sizes = [rows * t // sum(TAIL) for t in TAIL]
        for k in range(LAYERS):
            if k == 0:
                got = [jnp.concatenate([swap(g, "col", 1) for g in give0], axis=0)]
            elif k < LAST:
                give = users_dot(adj_oth, panel)
                got = [swap(give, "col", 1)]
            else:
                got, give, at = [], [], 0
                for n in sizes:
                    give.append(users_dot(adj_oth, panel, at, n))
                    got.append(swap(give[-1], "col", 1))
                    at += n
                oth, _ = lax.optimization_barrier((oth, give[-1]))
                give = jnp.concatenate(give, axis=0)
            mine = mine0 if k == 0 else users_dot(adj_own, panel)
            part = items_dot(adj_own, own, jnp.zeros((items, dim), f32))
            part = items_dot(adj_oth, oth, part)
            item = scatter_rows(part).astype(bf16)
            item_list.append(item)
            if k < LAST:
                own = (mine + got[0]).astype(bf16)
                own_list.append(own)
                oth = swap(own, "col", 1)
                oth_list.append(oth)
                panel = gather_items(item)

        def mean(parts):
            total = parts[0].astype(f32)
            for p in parts[1:]:
                total = total + p.astype(f32)
            return (total / (LAYERS + 1)).astype(bf16)

        out_item = mean(item_list)

        def inside(ids, base, n):
            local = ids - base
            return (local >= 0) & (local < n), jnp.clip(local, 0, n - 1)

        user_ids = triples[:, 0]
        block = row_idx * col_count * rows
        own_in, own_at = inside(user_ids, block + own_base, rows)
        oth_in, oth_at = inside(user_ids, block + oth_base, rows)

        def add_up(parts):
            total = parts[0].astype(f32)
            for p in parts[1:]:
                total = total + p.astype(f32)
            return total

        own_id = jnp.where(own_in, own_at, -1)
        oth_id = jnp.where(oth_in, oth_at, -1)
        both = pick_rows(own_id, oth_id, [mine] + own_list, [give] + oth_list)
        picked = scatter_rows(both)
        part_rows = picked[:, :dim]
        last_rows = (part_rows + cross(part_rows)).astype(bf16)
        user_vec = mean([picked[:, dim:], last_rows]).astype(f32)
        table = gather_items(out_item)
        share = count // row_count
        mine_ids = lax.dynamic_slice(triples, (row_idx * share, 0), (share, 3))
        item_in, item_at = inside(mine_ids[:, 1:].T.reshape(-1), col_idx * items, items)
        item_vec = jnp.take(table, item_at, axis=0).astype(f32).reshape(2, share, dim)
        dots = jnp.sum(user_vec[None] * item_vec, axis=2)
        dots = jnp.where(item_in.reshape(2, share), dots, 0.0)
        dots = dots + cross(dots)
        loss_sum = jnp.sum(jax.nn.softplus(dots[1] - dots[0])).reshape(1)
        loss_sum = loss_sum + swap(loss_sum, "row", 1)
        other_sum = swap(loss_sum, "row", 2)
        bpr_loss = ((loss_sum + other_sum) / count).reshape(())

        got[-2], bpr_loss = lax.optimization_barrier((got[-2], bpr_loss))
        at = 0
        out_user = None
        for i, n in enumerate(sizes):
            if i == len(sizes) - 1:
                break
            last = (mine[at:at + n] + got[i]).astype(bf16)
            piece = mean([t[at:at + n] for t in own_list] + [last])
            if out_user is None:
                out_user = jnp.pad(piece, ((0, rows - n), (0, 0)))
            else:
                out_user = lax.dynamic_update_slice(out_user, piece, (at, 0))
            at += n
        n = sizes[-1]
        out_user = finish(out_user, mine[rows - n:], got[-1], add_up([t[rows - n:] for t in own_list]))
        return out_user, out_item, bpr_loss

    return jax.shard_map(local_prog, mesh=mesh, in_specs=(P("row", "col"), P(("row", "col"), None), P(("col", "row"), None), P(None, None)), out_specs=(P(("row", "col"), None), P(("col", "row"), None), P()), check_vma=False)
```
